128 devices in a mesh: mx: 4 (over z), my: 4 (over y_hi, core), col: 8 (over y_lo, x).
Axes of the slice: x: 4, y: 4 (y_hi: 2, y_lo: 2; y = y_hi * 2 + y_lo), z: 4, core: 2. Of those that a mesh axis runs over, the one named last changes fastest.
Arguments:
- spectrum: float32 [2, 16, 128, 32, 512], P(None, 'col', None, 'mx', 'my'), may hold values from -6 to 6
- core_tensor: float32 [2, 64, 64, 16, 16, 16], P(None, 'col', None, ('mx', 'my')), may hold values from -0.01171875 to 0.01171875
- input_factor: float32 [128, 64], replicated, may hold values from -0.5 to 0.5
- output_factor: float32 [128, 64], replicated, may hold values from -0.75 to 0.75
- first_factor: float32 [32, 16], P('mx'), may hold values from -5 to 5
- second_factor: float32 [32, 16], P('my'), may hold values from -5 to 5
- third_factor: float32 [16, 16], replicated, may hold values from -5 to 5
Outputs:
- mixed_modes: float32 [2, 16, 128, 32, 512], P(None, 'col', None, 'mx', 'my')
The draws below stay inside these ranges and needn't reach their ends.
All inputs are finite; a program needn't handle non-finite values.
Results may differ from the reference program's by a relative error of at most 0.00007.
Values sent between devices are 32-bit elements; how exact they have to be, the bound alone decides.
No kernel may reach another device: no remote copies, remote signals or barrier semaphores. Data moves between devices by JAX's collectives and lax.ppermute only.
A program may use at most 128 MiB of HBM per device.

```python
import jax
import jax.numpy as jnp
from jax import lax

CIN = 128
COUT = 128
R1 = 64
R2 = 64
R3 = 16
R4 = 16
R5 = 16
KX = 32
KY = 32
KZ = 16
BATCH = 16


def block_scale(key, extent, split, low, largest):
    level, own = 1.0, jax.random.fold_in(key, 6)
    for dim, blocks in split:
        steps = jnp.exp(jax.random.uniform(jax.random.fold_in(own, dim), (blocks,), jnp.float32, low / len(split), largest / len(split)))
        level = level * jnp.repeat(steps, extent[dim] // blocks).reshape([-1 if axis == dim else 1 for axis in range(len(extent))])
    return level


def bell_draw(own_key, shape, width, most, split=(), held_as=jnp.bfloat16):
    values = width * jax.random.normal(own_key, shape, jnp.float32)
    if split:
        values = values * block_scale(own_key, shape, split, -0.22, 0.18)
    return jnp.clip(values, -most, most).astype(held_as)


def setup_inputs(seed: int = 0) -> dict:
    arg_keys = jax.random.split(jax.random.key(seed), 8)
    spectrum = bell_draw(arg_keys[0], (2, BATCH, CIN, KX, KY * KZ), 1.0, 6.0, ((1, 8), (3, 4), (4, 4)), jnp.float32)
    core_tensor = bell_draw(arg_keys[1], (2, R1, R2, R3, R4, R5), (R1 * R3 * R4 * R5) ** -0.5, 0.01171875, ((1, 8), (3, 16)), jnp.float32)
    input_factor = bell_draw(arg_keys[2], (CIN, R1), CIN ** -0.5, 0.5, (), jnp.float32)
    output_factor = bell_draw(arg_keys[3], (COUT, R2), R2 ** -0.5, 0.75, (), jnp.float32)
    first_factor = bell_draw(arg_keys[4], (KX, R3), 1.0, 5.0, ((0, 4),), jnp.float32)
    second_factor = bell_draw(arg_keys[5], (KY, R4), 1.0, 5.0, ((0, 4),), jnp.float32)
    third_factor = bell_draw(arg_keys[6], (KZ, R5), 1.0, 5.0, (), jnp.float32)
    return {"spectrum": spectrum, "core_tensor": core_tensor, "input_factor": input_factor, "output_factor": output_factor, "first_factor": first_factor, "second_factor": second_factor, "third_factor": third_factor}


def reference(spectrum, core_tensor, input_factor, output_factor, first_factor, second_factor, third_factor):
    precise = lax.Precision.HIGHEST
    rank_spectrum = jnp.einsum('cbikm,ir->cbrkm', spectrum, input_factor, precision=precise)
    core_third = jnp.einsum('cpqstu,zu->cpqstz', core_tensor, third_factor, precision=precise)
    core_second = jnp.einsum('cpqstz,yt->cpqsyz', core_third, second_factor, precision=precise)
    core_second = core_second.reshape(2, R1, R2, R3, KY * KZ)

    def per_mode_row(inputs):
        spectrum_row, factor_row = inputs
        weight_row = jnp.einsum('cpqsm,s->cpqm', core_second, factor_row, precision=precise)
        real_part = jnp.einsum('brm,rqm->bqm', spectrum_row[0], weight_row[0], precision=precise) - jnp.einsum('brm,rqm->bqm', spectrum_row[1], weight_row[1], precision=precise)
        imag_part = jnp.einsum('brm,rqm->bqm', spectrum_row[0], weight_row[1], precision=precise) + jnp.einsum('brm,rqm->bqm', spectrum_row[1], weight_row[0], precision=precise)
        mode_values = jnp.stack([real_part, imag_part])
        return jnp.einsum('oq,cbqm->cbom', output_factor, mode_values, precision=precise)

    mixed_rows = lax.map(per_mode_row, (jnp.moveaxis(rank_spectrum, 3, 0), first_factor))
    return jnp.moveaxis(mixed_rows, 0, 3)
```

```python
import functools

import jax
import jax.numpy as jnp
from jax import lax
from jax.experimental import pallas as pl
from jax.experimental.pallas import tpu as pltpu
from jax.sharding import PartitionSpec as P

precise = lax.Precision.HIGHEST
LANES = 128


def dot(a, b, contract=(1, 0)):
    return lax.dot_general(
        a, b, (((contract[0],), (contract[1],)), ((), ())),
        precision=precise, preferred_element_type=jnp.float32,
    )


def iota(shape, dim):
    return lax.broadcasted_iota(jnp.int32, shape, dim)


def core_kernel(core_ref, second_ref, third_ref, out_ref, mat_ref):
    @pl.when(pl.program_id(0) == 0)
    def _():
        def picks(width):
            row, col = iota((512, width), 0), iota((512, width), 1)
            c, b, a, r = row & 7, (row >> 3) & 3, (row >> 5) & 3, row >> 7
            return col, 8 * b + 2 * r + (a >> 1), (a & 1) * 8 + c

        col, ky, _ = picks(second_ref.shape[0])
        rows_y = dot((col == ky).astype(jnp.float32), second_ref[...])
        col, _, kz = picks(third_ref.shape[0])
        rows_z = dot((col == kz).astype(jnp.float32), third_ref[...])
        of_t = (iota((16, 256), 1) >> 4 == iota((16, 256), 0)).astype(jnp.float32)
        of_u = (iota((16, 256), 1) & 15 == iota((16, 256), 0)).astype(jnp.float32)
        mat_ref[...] = dot(rows_y, of_t) * dot(rows_z, of_u)

    both = jnp.concatenate([core_ref[0, 0], core_ref[0, 1], core_ref[1, 0], core_ref[1, 1]], axis=1)
    out = dot(mat_ref[...], both)
    for part in range(2):
        for r in range(4):
            out_ref[pl.ds(part * 4 + r, 128, stride=8), :] = out[
                r * 128 : (r + 1) * 128, part * LANES : (part + 1) * LANES
            ]


def core_chunks(core, second, third):
    return pl.pallas_call(
        core_kernel,
        grid=(4,),
        in_specs=[
            pl.BlockSpec((2, 2, 256, 64), lambda i: (0, i, 0, 0)),
            pl.BlockSpec(second.shape, lambda i: (0, 0)),
            pl.BlockSpec(third.shape, lambda i: (0, 0)),
        ],
        out_specs=pl.BlockSpec((1024, LANES), lambda i: (0, i)),
        out_shape=jax.ShapeDtypeStruct((1024, 512), jnp.float32),
        scratch_shapes=[pltpu.VMEM((512, 256), jnp.float32)],
        name="core_chunks",
    )(core, second, third)


def spectrum_kernel(spec_ref, factor_ref, out_ref):
    factor = factor_ref[...]
    for k in range(8):
        halves = [dot(factor, spec_ref[0, b, pl.ds(k, 128, stride=8), :]) for b in range(2)]
        turned = jnp.concatenate(halves, axis=0).T
        for r in range(4):
            out_ref[pl.ds(k * 4 + r, 32, stride=32), :] = turned[r * 32 : (r + 1) * 32]


def spectrum_chunks(spec, factor):
    return pl.pallas_call(
        spectrum_kernel,
        grid=(2,),
        in_specs=[
            pl.BlockSpec((1, 2, 1024, LANES), lambda i: (i, 0, 0, 0)),
            pl.BlockSpec((64, 128), lambda i: (0, 0)),
        ],
        out_specs=pl.BlockSpec((1024, LANES), lambda i: (0, i)),
        out_shape=jax.ShapeDtypeStruct((1024, 256), jnp.float32),
        name="spectrum_chunks",
    )(spec, factor)


def mode_kernel(core_ref, spec_ref, first_ref, out_ref, w_ref, x_ref, v_ref):
    of_s = (iota((128, 16), 0) >> 3 == iota((128, 16), 1)).astype(jnp.float32)
    of_k = ((iota((32, 256), 1) >> 2) & 31 == iota((32, 256), 0)).astype(jnp.float32)
    row, col = iota((128, 256), 0), iota((128, 256), 1)
    same = (((row >> 2) & 1) == (col >> 7)) & ((row & 3) == (col & 3))
    expand = jnp.where(same, dot(dot(of_s, first_ref[...], (1, 1)), of_k), 0.0)

    for src in range(8):
        for pair in range(4):
            block = core_ref[:, src, :, pair * LANES : (pair + 1) * LANES].reshape(128, LANES)
            w = dot(block.T, expand)
            for half in range(2):
                rows = w[half * 64 : (half + 1) * 64]
                p = src * 8 + pair * 2 + half
                w_ref[p, 0] = rows[:, :LANES]
                w_ref[p, 1] = rows[:, LANES:]
                w_ref[p, 2] = rows[:, :LANES] + rows[:, LANES:]

    for src in range(8):
        parts = [
            spec_ref[:, src, :, part * LANES : (part + 1) * LANES].reshape(128, LANES).T
            for part in range(2)
        ]
        parts.append(parts[0] + parts[1])
        for part in range(3):
            for b in range(2):
                x_ref[src * 2 + b, part] = parts[part][b * 64 : (b + 1) * 64]

    @pl.loop(0, 16)
    def _(step):
        samples, q0 = step // 4 * 4, pl.multiple_of(step % 4 * 16, 16)

        def one(p, sums):
            w = [w_ref[p, part, pl.ds(q0, 16), :] for part in range(3)]
            return tuple(
                sums[b * 3 + part] + x_ref[samples + b, part, pl.ds(p, 1), :] * w[part]
                for b in range(4)
                for part in range(3)
            )

        zero = jnp.zeros((16, LANES), jnp.float32)
        sums = lax.fori_loop(0, 64, one, (zero,) * 12, unroll=8)
        for b in range(4):
            rr, ii, mixed = sums[b * 3 : b * 3 + 3]
            v_ref[samples + b, 0, pl.ds(q0, 16), :] = rr - ii
            v_ref[samples + b, 1, pl.ds(q0, 16), :] = mixed - rr - ii

    for src in range(8):
        for part in range(2):
            both = jnp.concatenate([v_ref[src * 2, part], v_ref[src * 2 + 1, part]], axis=0)
            out_ref[:, src, :, part * LANES : (part + 1) * LANES] = both.T.reshape(4, 32, LANES)


def mode_products(core, spec, first):
    return pl.pallas_call(
        mode_kernel,
        out_shape=jax.ShapeDtypeStruct((4, 8, 32, 256), jnp.float32),
        scratch_shapes=[
            pltpu.VMEM((64, 3, 64, LANES), jnp.float32),
            pltpu.VMEM((16, 3, 64, LANES), jnp.float32),
            pltpu.VMEM((16, 2, 64, LANES), jnp.float32),
        ],
        name="mode_products",
    )(core, spec, first)


def output_kernel(value_ref, factor_ref, out_ref):
    factor = factor_ref[...].T
    for k in range(8):
        rows = [value_ref[pl.ds(k * 4 + r, 32, stride=32), :] for r in range(4)]
        turned = jnp.concatenate(rows, axis=0).T
        for b in range(2):
            out_ref[0, b, pl.ds(k, 128, stride=8), :] = dot(factor, turned[b * 64 : (b + 1) * 64])


def output_modes(values, factor):
    return pl.pallas_call(
        output_kernel,
        grid=(2,),
        in_specs=[
            pl.BlockSpec((1024, LANES), lambda i: (0, i)),
            pl.BlockSpec((64, 128), lambda i: (0, 0)),
        ],
        out_specs=pl.BlockSpec((1, 2, 1024, LANES), lambda i: (i, 0, 0, 0)),
        out_shape=jax.ShapeDtypeStruct((2, 2, 1024, LANES), jnp.float32),
        name="output_modes",
    )(values, factor)


def swap(chunks, axes):
    return lax.all_to_all(chunks, axes, split_axis=0, concat_axis=0, tiled=True)


def per_device(
    spectrum, core_tensor, input_factor, output_factor, first_factor, second_factor, third_factor
):
    second = lax.all_gather(second_factor, "my", axis=0, tiled=True)
    first = lax.all_gather(first_factor, "mx", axis=0, tiled=True)
    core = jnp.transpose(core_tensor, (0, 1, 3, 4, 5, 2)).reshape(2, 8, 256, 64)
    core = core_chunks(core, second, third_factor)
    core = swap(core.reshape(128, 8, 512), ("mx", "my", "col"))
    spec = spectrum_chunks(spectrum.reshape(2, 2, 1024, LANES), input_factor.T)
    spec = swap(spec.reshape(32, 32, 256), ("mx", "col"))
    values = mode_products(core.reshape(16, 8, 8, 512), spec.reshape(4, 8, 32, 256), first)
    values = swap(values.reshape(32, 32, 256), ("mx", "col"))
    out = output_modes(values.reshape(1024, 256), output_factor.T)
    return out.reshape(spectrum.shape)


def solution(mesh):
    placed = (
        P(None, "col", None, "mx", "my"),
        P(None, "col", None, ("mx", "my"), None, None),
        P(),
        P(),
        P("mx", None),
        P("my", None),
        P(),
    )
    return jax.shard_map(
        per_device,
        mesh=mesh,
        in_specs=placed,
        out_specs=P(None, "col", None, "mx", "my"),
        check_vma=False,
    )
```

```python
import functools

import jax
import jax.numpy as jnp
from jax import lax
from jax.experimental import pallas as pl
from jax.experimental.pallas import tpu as pltpu
from jax.sharding import PartitionSpec as P

LANES = 128
VMEM_SMALL = 16 * 2**20
VMEM_LARGE = 32 * 2**20


def dot(a, b):
    return jnp.dot(a, b, preferred_element_type=jnp.float32)


def split(x):
    high = x.astype(jnp.bfloat16)
    return high, (x - high.astype(jnp.float32)).astype(jnp.bfloat16)


def split3(x):
    high, rest = x.astype(jnp.bfloat16), None
    rest = x - high.astype(jnp.float32)
    return (high, *split(rest))


def iota(shape, dim):
    return lax.broadcasted_iota(jnp.int32, shape, dim)


def pick(chosen, table):
    one = chosen.astype(jnp.bfloat16)
    high, mid, low = split3(table)
    return (dot(one, high) + dot(one, mid)) + dot(one, low)


def pick_lanes(table, chosen):
    one = chosen.astype(jnp.bfloat16)
    high, mid, low = split3(table)
    return (dot(high, one) + dot(mid, one)) + dot(low, one)


def core_kernel(core_ref, factors_ref, third_ref, out_ref, mat_ref):
    @pl.when(pl.program_id(0) == 0)
    def _():
        def place(width):
            row, col = iota((512, width), 0), iota((512, width), 1)
            c, b, a, r = row & 7, (row >> 3) & 3, (row >> 5) & 3, row >> 7
            return col, 8 * b + 2 * r + (a >> 1), (a & 1) * 8 + c

        of_t = iota((16, 256), 1) >> 4 == iota((16, 256), 0)
        of_u = iota((16, 256), 1) & 15 == iota((16, 256), 0)
        second = pick_lanes(factors_ref[:32, 16:32], of_t)
        third = pick_lanes(third_ref[...], of_u)
        col, ky, _ = place(32)
        by_y = pick(col == ky, second)
        col, _, kz = place(16)
        mat = by_y * pick(col == kz, third)
        mat_ref[0], mat_ref[1] = split(mat)

    both = jnp.concatenate([core_ref[0, 0], core_ref[0, 1], core_ref[1, 0], core_ref[1, 1]], axis=1)
    high, low = split(both)
    out = dot(mat_ref[0], high) + dot(mat_ref[0], low) + dot(mat_ref[1], high)
    for part in range(2):
        for r in range(4):
            out_ref[pl.ds(part * 4 + r, 128, stride=8), :] = out[
                r * 128 : (r + 1) * 128, part * LANES : (part + 1) * LANES
            ]


def core_chunks(core, factors, third):
    return pl.pallas_call(
        core_kernel,
        grid=(4,),
        in_specs=[
            pl.BlockSpec((2, 2, 256, 64), lambda i: (0, i, 0, 0)),
            pl.BlockSpec((128, LANES), lambda i: (0, 0)),
            pl.BlockSpec(third.shape, lambda i: (0, 0)),
        ],
        out_specs=pl.BlockSpec((1024, LANES), lambda i: (0, i)),
        out_shape=jax.ShapeDtypeStruct((1024, 512), jnp.float32),
        scratch_shapes=[pltpu.VMEM((2, 512, 256), jnp.bfloat16)],
        compiler_params=pltpu.CompilerParams(vmem_limit_bytes=VMEM_SMALL),
        name="core_chunks",
    )(core, factors, third)


def spectrum_kernel(spec_ref, factor_ref, out_ref):
    high, low = split(factor_ref[...])
    rows = jnp.concatenate(
        [jnp.concatenate([high, high], axis=1), jnp.concatenate([low, low], axis=1)], axis=0
    )
    for k in range(8):
        both = jnp.concatenate(
            [spec_ref[0, b, pl.ds(k, 128, stride=8), :] for b in range(2)], axis=1
        )
        out = dot(rows, jnp.concatenate(split(both), axis=0))
        out = out[:64] + out[64:]
        turned = jnp.concatenate([out[:, :LANES], out[:, LANES:]], axis=0).T
        for r in range(4):
            out_ref[pl.ds(k * 4 + r, 32, stride=32), :] = turned[r * 32 : (r + 1) * 32]


def spectrum_chunks(spec, factor):
    return pl.pallas_call(
        spectrum_kernel,
        grid=(2,),
        in_specs=[
            pl.BlockSpec((1, 2, 1024, LANES), lambda i: (i, 0, 0, 0)),
            pl.BlockSpec((64, 128), lambda i: (0, 0)),
        ],
        out_specs=pl.BlockSpec((1024, LANES), lambda i: (0, i)),
        out_shape=jax.ShapeDtypeStruct((1024, 256), jnp.float32),
        compiler_params=pltpu.CompilerParams(vmem_limit_bytes=VMEM_SMALL),
        name="spectrum_chunks",
    )(spec, factor)


def mode_kernel(core_ref, spec_ref, factors_ref, out_ref, w_ref, x_ref, v_ref):
    of_s = iota((128, 16), 0) >> 3 == iota((128, 16), 1)
    kx = (iota((128, 256), 1) >> 2) & 31
    of_k = (kx >> 3) * 32 + (kx & 7) == iota((128, 256), 0)
    row, col = iota((128, 256), 0), iota((128, 256), 1)
    same = (((row >> 2) & 1) == (col >> 7)) & ((row & 3) == (col & 3))
    first = pick_lanes(factors_ref[...].T[:16], of_k)
    expand = jnp.where(same, pick(of_s, first), 0.0)
    high, low = split(expand)
    expand_high = jnp.concatenate([high, high], axis=0)
    expand_low = jnp.concatenate([low, low], axis=0)

    for src in range(8):
        for pair in range(4):
            block = core_ref[:, src, :, pair * LANES : (pair + 1) * LANES].reshape(128, LANES)
            turned = jnp.concatenate(split(block.T), axis=1)
            w = dot(turned, expand_high) + dot(turned, expand_low)
            for half in range(2):
                rows = w[half * 64 : (half + 1) * 64]
                p = src * 8 + pair * 2 + half
                w_ref[p, 0] = rows[:, :LANES]
                w_ref[p, 1] = rows[:, LANES:]
                w_ref[p, 2] = rows[:, :LANES] + rows[:, LANES:]

    for src in range(8):
        parts = [
            spec_ref[:, src, :, part * LANES : (part + 1) * LANES].reshape(128, LANES).T
            for part in range(2)
        ]
        parts.append(parts[0] + parts[1])
        for part in range(3):
            for b in range(2):
                x_ref[src * 2 + b, part] = parts[part][b * 64 : (b + 1) * 64]

    @pl.loop(0, 16)
    def _(step):
        samples, q0 = step // 4 * 4, pl.multiple_of(step % 4 * 16, 16)

        def one(p, sums):
            w = [w_ref[p, part, pl.ds(q0, 16), :] for part in range(3)]
            return tuple(
                sums[b * 3 + part] + x_ref[samples + b, part, pl.ds(p, 1), :] * w[part]
                for b in range(4)
                for part in range(3)
            )

        zero = jnp.zeros((16, LANES), jnp.float32)
        sums = lax.fori_loop(0, 64, one, (zero,) * 12, unroll=8)
        for b in range(4):
            rr, ii, mixed = sums[b * 3 : b * 3 + 3]
            v_ref[samples + b, 0, pl.ds(q0, 16), :] = rr - ii
            v_ref[samples + b, 1, pl.ds(q0, 16), :] = mixed - rr - ii

    for src in range(8):
        for part in range(2):
            both = jnp.concatenate([v_ref[src * 2, part], v_ref[src * 2 + 1, part]], axis=0)
            out_ref[:, src, :, part * LANES : (part + 1) * LANES] = both.T.reshape(4, 32, LANES)


def mode_products(core, spec, factors):
    return pl.pallas_call(
        mode_kernel,
        out_shape=jax.ShapeDtypeStruct((4, 8, 32, 256), jnp.float32),
        scratch_shapes=[
            pltpu.VMEM((64, 3, 64, LANES), jnp.float32),
            pltpu.VMEM((16, 3, 64, LANES), jnp.float32),
            pltpu.VMEM((16, 2, 64, LANES), jnp.float32),
        ],
        compiler_params=pltpu.CompilerParams(vmem_limit_bytes=VMEM_LARGE),
        name="mode_products",
    )(core, spec, factors)


def output_kernel(value_ref, factor_ref, out_ref):
    high, low = split(factor_ref[...].T)
    factor = jnp.concatenate([high, high, low, low], axis=1)
    for k in range(8):
        rows = [value_ref[pl.ds(k * 4 + r, 32, stride=32), :] for r in range(4)]
        turned = jnp.concatenate(rows, axis=0).T
        turned = jnp.concatenate([turned[:64], turned[64:]], axis=1)
        high, low = split(turned)
        out = dot(factor, jnp.concatenate([high, low, high, low], axis=0))
        for b in range(2):
            out_ref[0, b, pl.ds(k, 128, stride=8), :] = out[:, b * LANES : (b + 1) * LANES]


def output_modes(values, factor):
    return pl.pallas_call(
        output_kernel,
        grid=(2,),
        in_specs=[
            pl.BlockSpec((1024, LANES), lambda i: (0, i)),
            pl.BlockSpec((64, 128), lambda i: (0, 0)),
        ],
        out_specs=pl.BlockSpec((1, 2, 1024, LANES), lambda i: (i, 0, 0, 0)),
        out_shape=jax.ShapeDtypeStruct((2, 2, 1024, LANES), jnp.float32),
        compiler_params=pltpu.CompilerParams(vmem_limit_bytes=VMEM_SMALL),
        name="output_modes",
    )(values, factor)


def swap(chunks, axes):
    return lax.all_to_all(chunks, axes, split_axis=0, concat_axis=0, tiled=True)


def per_device(
    spectrum, core_tensor, input_factor, output_factor, first_factor, second_factor, third_factor
):
    mine = jnp.concatenate(
        [first_factor, second_factor, jnp.zeros((8, LANES - 32), jnp.float32)], axis=1
    )
    factors = swap(jnp.broadcast_to(mine, (16, 8, LANES)), ("mx", "my")).reshape(128, LANES)
    core = jnp.transpose(core_tensor, (0, 1, 3, 4, 5, 2)).reshape(2, 8, 256, 64)
    core = core_chunks(core, factors, third_factor)
    core = swap(core.reshape(128, 8, 512), ("mx", "my", "col"))
    spec = spectrum_chunks(spectrum.reshape(2, 2, 1024, LANES), input_factor.T)
    spec = swap(spec.reshape(32, 32, 256), ("mx", "col"))
    values = mode_products(core.reshape(16, 8, 8, 512), spec.reshape(4, 8, 32, 256), factors)
    values = swap(values.reshape(32, 32, 256), ("mx", "col"))
    out = output_modes(values.reshape(1024, 256), output_factor.T)
    return out.reshape(spectrum.shape)


def solution(mesh):
    placed = (
        P(None, "col", None, "mx", "my"),
        P(None, "col", None, ("mx", "my"), None, None),
        P(),
        P(),
        P("mx", None),
        P("my", None),
        P(),
    )
    return jax.shard_map(
        per_device,
        mesh=mesh,
        in_specs=placed,
        out_specs=P(None, "col", None, "mx", "my"),
        check_vma=False,
    )
```

```python
import jax
import jax.numpy as jnp
from jax import lax
from jax.experimental import pallas as pl
from jax.experimental.pallas import tpu as pltpu
from jax.sharding import PartitionSpec as P


LANES = 128
VMEM_SMALL = 16 * 2**20
VMEM_LARGE = 32 * 2**20
VMEM_ALONE = 61 * 2**20


def dot(a, b):
    return jnp.dot(a, b, preferred_element_type=jnp.float32)


def split(x):
    high = x.astype(jnp.bfloat16)
    return high, (x - high.astype(jnp.float32)).astype(jnp.bfloat16)


def split3(x):
    high, rest = x.astype(jnp.bfloat16), None
    rest = x - high.astype(jnp.float32)
    return (high, *split(rest))


def iota(shape, dim):
    return lax.broadcasted_iota(jnp.int32, shape, dim)


def pick(chosen, table):
    one = chosen.astype(jnp.bfloat16)
    high, mid, low = split3(table)
    return (dot(one, high) + dot(one, mid)) + dot(one, low)


def pick_lanes(table, chosen):
    one = chosen.astype(jnp.bfloat16)
    high, mid, low = split3(table)
    return (dot(high, one) + dot(mid, one)) + dot(low, one)


def core_kernel(core_ref, second_ref, third_ref, out_ref, mat_ref):
    @pl.when(pl.program_id(0) == 0)
    def _():
        def place(width):
            row, col = iota((512, width), 0), iota((512, width), 1)
            c, b, a, r = row & 7, (row >> 3) & 3, (row >> 5) & 3, row >> 7
            return col, 8 * b + 2 * r + (a >> 1), (a & 1) * 8 + c

        of_t = iota((16, 256), 1) >> 4 == iota((16, 256), 0)
        of_u = iota((16, 256), 1) & 15 == iota((16, 256), 0)
        second = pick_lanes(second_ref[...], of_t)
        third = pick_lanes(third_ref[...], of_u)
        col, ky, _ = place(32)
        by_y = pick(col == ky, second)
        col, _, kz = place(16)
        mat = by_y * pick(col == kz, third)
        mat_ref[0], mat_ref[1] = split(mat)

    both = jnp.concatenate([core_ref[0, 0], core_ref[0, 1], core_ref[1, 0], core_ref[1, 1]], axis=1)
    high, low = split(both)
    out = dot(mat_ref[0], high) + dot(mat_ref[0], low) + dot(mat_ref[1], high)
    for part in range(2):
        for r in range(4):
            out_ref[pl.ds(part * 4 + r, 128, stride=8), :] = out[
                r * 128 : (r + 1) * 128, part * LANES : (part + 1) * LANES
            ]


def core_chunks(core, second, third):
    return pl.pallas_call(
        core_kernel,
        grid=(4,),
        in_specs=[
            pl.BlockSpec((2, 2, 256, 64), lambda i: (0, i, 0, 0)),
            pl.BlockSpec(second.shape, lambda i: (0, 0)),
            pl.BlockSpec(third.shape, lambda i: (0, 0)),
        ],
        out_specs=pl.BlockSpec((1024, LANES), lambda i: (0, i)),
        out_shape=jax.ShapeDtypeStruct((1024, 512), jnp.float32),
        scratch_shapes=[pltpu.VMEM((2, 512, 256), jnp.bfloat16)],
        compiler_params=pltpu.CompilerParams(vmem_limit_bytes=VMEM_ALONE),
        name="core_chunks",
    )(core, second, third)


def spectrum_kernel(spec_hbm, factor_ref, first_ref, out_ref, spec_ref, sems):
    copies = [
        pltpu.make_async_copy(spec_hbm.at[part, b], spec_ref.at[part, b], sems.at[part, b])
        for part in range(2)
        for b in range(2)
    ]
    for copy in copies:
        copy.start()
    high, low = split(factor_ref[...])
    rows = jnp.concatenate(
        [jnp.concatenate([high, high], axis=1), jnp.concatenate([low, low], axis=1)], axis=0
    )
    for part in range(2):
        copies[2 * part].wait()
        copies[2 * part + 1].wait()
        for k in range(8):
            both = jnp.concatenate(
                [spec_ref[part, b, pl.ds(k, 128, stride=8), :] for b in range(2)], axis=1
            )
            out = dot(rows, jnp.concatenate(split(both), axis=0))
            out = out[:64] + out[64:]
            turned = jnp.concatenate([out[:, :LANES], out[:, LANES:]], axis=0).T
            for r in range(4):
                row = part * 32 + k * 4 + r
                out_ref[pl.ds(row, 32, stride=72), :] = turned[r * 32 : (r + 1) * 32]
    first = jnp.concatenate([first_ref[...], jnp.zeros((8, LANES - 16), jnp.float32)], axis=1)
    for k in range(8):
        out_ref[pl.ds(64 + k, 32, stride=72), :] = jnp.broadcast_to(first[k : k + 1], (32, LANES))


def spectrum_chunks(spec, factor, first):
    return pl.pallas_call(
        spectrum_kernel,
        in_specs=[
            pl.BlockSpec(memory_space=pltpu.MemorySpace.HBM),
            pl.BlockSpec(memory_space=pltpu.VMEM),
            pl.BlockSpec(memory_space=pltpu.VMEM),
        ],
        scratch_shapes=[
            pltpu.VMEM((2, 2, 1024, LANES), jnp.float32),
            pltpu.SemaphoreType.DMA((2, 2)),
        ],
        out_shape=jax.ShapeDtypeStruct((32 * 72, LANES), jnp.float32),
        compiler_params=pltpu.CompilerParams(vmem_limit_bytes=VMEM_ALONE),
        name="spectrum_chunks",
    )(spec, factor, first)


def mode_kernel(core_ref, spec_ref, out_ref, w_ref, x_ref, v_ref):
    of_s = iota((128, 16), 0) >> 3 == iota((128, 16), 1)
    of_k = (iota((LANES, 256), 1) >> 2) & 31 == iota((LANES, 256), 0)
    row, col = iota((128, 256), 0), iota((128, 256), 1)
    same = (((row >> 2) & 1) == (col >> 7)) & ((row & 3) == (col & 3))
    first = [spec_ref[a, 0, 64:72, :] for a in range(4)]
    first = jnp.concatenate(first + [jnp.zeros((96, LANES), jnp.float32)], axis=0)
    first = pick_lanes(first.T[:16], of_k)
    expand = jnp.where(same, pick(of_s, first), 0.0)
    high, low = split(expand)
    expand_high = jnp.concatenate([high, high], axis=0)
    expand_low = jnp.concatenate([low, low], axis=0)

    for src in range(8):
        for pair in range(4):
            block = core_ref[:, src, :, pair * LANES : (pair + 1) * LANES].reshape(128, LANES)
            turned = jnp.concatenate(split(block.T), axis=1)
            w = dot(turned, expand_high) + dot(turned, expand_low)
            for half in range(2):
                rows = w[half * 64 : (half + 1) * 64]
                p = src * 8 + pair * 2 + half
                w_ref[p, 0] = rows[:, :LANES]
                w_ref[p, 1] = rows[:, LANES:]
                w_ref[p, 2] = rows[:, :LANES] + rows[:, LANES:]

    for src in range(8):
        parts = [
            spec_ref[:, src, part * 32 : (part + 1) * 32, :].reshape(128, LANES).T
            for part in range(2)
        ]
        parts.append(parts[0] + parts[1])
        for part in range(3):
            for b in range(2):
                x_ref[src * 2 + b, part] = parts[part][b * 64 : (b + 1) * 64]

    @pl.loop(0, 16)
    def _(step):
        samples, q0 = step // 4 * 4, pl.multiple_of(step % 4 * 16, 16)

        def one(p, sums):
            w = [w_ref[p, part, pl.ds(q0, 16), :] for part in range(3)]
            return tuple(
                sums[b * 3 + part] + x_ref[samples + b, part, pl.ds(p, 1), :] * w[part]
                for b in range(4)
                for part in range(3)
            )

        zero = jnp.zeros((16, LANES), jnp.float32)
        sums = lax.fori_loop(0, 64, one, (zero,) * 12, unroll=8)
        for b in range(4):
            rr, ii, mixed = sums[b * 3 : b * 3 + 3]
            v_ref[samples + b, 0, pl.ds(q0, 16), :] = rr - ii
            v_ref[samples + b, 1, pl.ds(q0, 16), :] = mixed - rr - ii

    for src in range(8):
        for part in range(2):
            both = jnp.concatenate([v_ref[src * 2, part], v_ref[src * 2 + 1, part]], axis=0)
            out_ref[:, src, :, part * LANES : (part + 1) * LANES] = both.T.reshape(4, 32, LANES)


def mode_products(core, spec):
    return pl.pallas_call(
        mode_kernel,
        out_shape=jax.ShapeDtypeStruct((4, 8, 32, 256), jnp.float32),
        scratch_shapes=[
            pltpu.VMEM((64, 3, 64, LANES), jnp.float32),
            pltpu.VMEM((16, 3, 64, LANES), jnp.float32),
            pltpu.VMEM((16, 2, 64, LANES), jnp.float32),
        ],
        compiler_params=pltpu.CompilerParams(vmem_limit_bytes=VMEM_LARGE),
        name="mode_products",
    )(core, spec)


def output_kernel(value_ref, factor_ref, out_ref):
    high, low = split(factor_ref[...].T)
    factor = jnp.concatenate([high, high, low, low], axis=1)
    for k in range(8):
        rows = [value_ref[pl.ds(k * 4 + r, 32, stride=32), :] for r in range(4)]
        turned = jnp.concatenate(rows, axis=0).T
        turned = jnp.concatenate([turned[:64], turned[64:]], axis=1)
        high, low = split(turned)
        out = dot(factor, jnp.concatenate([high, low, high, low], axis=0))
        for b in range(2):
            out_ref[0, b, pl.ds(k, 128, stride=8), :] = out[:, b * LANES : (b + 1) * LANES]


def output_modes(values, factor):
    return pl.pallas_call(
        output_kernel,
        grid=(2,),
        in_specs=[
            pl.BlockSpec((1024, LANES), lambda i: (0, i)),
            pl.BlockSpec((64, 128), lambda i: (0, 0)),
        ],
        out_specs=pl.BlockSpec((1, 2, 1024, LANES), lambda i: (i, 0, 0, 0)),
        out_shape=jax.ShapeDtypeStruct((2, 2, 1024, LANES), jnp.float32),
        compiler_params=pltpu.CompilerParams(vmem_limit_bytes=VMEM_SMALL),
        name="output_modes",
    )(values, factor)


def swap(chunks, axes):
    return lax.all_to_all(chunks, axes, split_axis=0, concat_axis=0, tiled=True)


def per_device(
    spectrum, core_tensor, input_factor, output_factor, first_factor, second_factor, third_factor
):
    spec = spectrum_chunks(spectrum.reshape(2, 2, 1024, LANES), input_factor.T, first_factor)
    spec = swap(spec.reshape(32, 72, LANES), ("mx", "col"))
    second = lax.all_gather(second_factor, "my", axis=0, tiled=True)
    core = jnp.transpose(core_tensor, (0, 1, 3, 4, 5, 2)).reshape(2, 8, 256, 64)
    core = core_chunks(core, second, third_factor)
    core = swap(core.reshape(128, 8, 512), ("mx", "my", "col"))
    values = mode_products(core.reshape(16, 8, 8, 512), spec.reshape(4, 8, 72, LANES))
    values = swap(values.reshape(32, 32, 256), ("mx", "col"))
    out = output_modes(values.reshape(1024, 256), output_factor.T)
    return out.reshape(spectrum.shape)


def solution(mesh):
    placed = (
        P(None, "col", None, "mx", "my"),
        P(None, "col", None, ("mx", "my"), None, None),
        P(),
        P(),
        P("mx", None),
        P("my", None),
        P(),
    )
    return jax.shard_map(
        per_device,
        mesh=mesh,
        in_specs=placed,
        out_specs=P(None, "col", None, "mx", "my"),
        check_vma=False,
    )
```

```python
import jax
import jax.numpy as jnp
from jax import lax
from jax.experimental import pallas as pl
from jax.experimental.pallas import tpu as pltpu
from jax.sharding import PartitionSpec as P


LANES = 128
VMEM_SMALL = 16 * 2**20
VMEM_LARGE = 32 * 2**20
VMEM_ALONE = 61 * 2**20


def dot(a, b):
    return jnp.dot(a, b, preferred_element_type=jnp.float32)


def split(x):
    high = x.astype(jnp.bfloat16)
    return high, (x - high.astype(jnp.float32)).astype(jnp.bfloat16)


def split3(x):
    high, rest = x.astype(jnp.bfloat16), None
    rest = x - high.astype(jnp.float32)
    return (high, *split(rest))


def iota(shape, dim):
    return lax.broadcasted_iota(jnp.int32, shape, dim)


def pick(chosen, table):
    one = chosen.astype(jnp.bfloat16)
    high, mid, low = split3(table)
    return (dot(one, high) + dot(one, mid)) + dot(one, low)


def pick_lanes(table, chosen):
    one = chosen.astype(jnp.bfloat16)
    high, mid, low = split3(table)
    return (dot(high, one) + dot(mid, one)) + dot(low, one)


def core_kernel(core_ref, second_ref, third_ref, out_ref, mat_ref):
    @pl.when(pl.program_id(0) == 0)
    def _():
        def place(width):
            row, col = iota((512, width), 0), iota((512, width), 1)
            c, b, a, r = row & 7, (row >> 3) & 3, (row >> 5) & 3, row >> 7
            return col, 8 * b + 2 * r + (a >> 1), (a & 1) * 8 + c

        of_t = iota((16, 256), 1) >> 4 == iota((16, 256), 0)
        of_u = iota((16, 256), 1) & 15 == iota((16, 256), 0)
        second = pick_lanes(second_ref[...], of_t)
        third = pick_lanes(third_ref[...], of_u)
        col, ky, _ = place(32)
        by_y = pick(col == ky, second)
        col, _, kz = place(16)
        mat = by_y * pick(col == kz, third)
        mat_ref[0], mat_ref[1] = split(mat)

    both = jnp.concatenate([core_ref[0, 0], core_ref[0, 1], core_ref[1, 0], core_ref[1, 1]], axis=1)
    high, low = split(both)
    out = dot(mat_ref[0], high) + dot(mat_ref[0], low) + dot(mat_ref[1], high)
    for part in range(2):
        for r in range(4):
            out_ref[pl.ds(part * 4 + r, 128, stride=8), :] = out[
                r * 128 : (r + 1) * 128, part * LANES : (part + 1) * LANES
            ]


def core_chunks(core, second, third):
    return pl.pallas_call(
        core_kernel,
        grid=(4,),
        in_specs=[
            pl.BlockSpec((2, 2, 256, 64), lambda i: (0, i, 0, 0)),
            pl.BlockSpec(second.shape, lambda i: (0, 0)),
            pl.BlockSpec(third.shape, lambda i: (0, 0)),
        ],
        out_specs=pl.BlockSpec((1024, LANES), lambda i: (0, i)),
        out_shape=jax.ShapeDtypeStruct((1024, 512), jnp.float32),
        scratch_shapes=[pltpu.VMEM((2, 512, 256), jnp.bfloat16)],
        compiler_params=pltpu.CompilerParams(vmem_limit_bytes=VMEM_ALONE),
        name="core_chunks",
    )(core, second, third)


def spectrum_kernel(spec_ref, factor_ref, first_ref, out_ref):
    high, low = split(factor_ref[...])
    rows = jnp.concatenate(
        [jnp.concatenate([high, high], axis=1), jnp.concatenate([low, low], axis=1)], axis=0
    )
    for part in range(2):
        for k in range(8):
            both = jnp.concatenate(
                [spec_ref[part, b, pl.ds(k, 128, stride=8), :] for b in range(2)], axis=1
            )
            out = dot(rows, jnp.concatenate(split(both), axis=0))
            out = out[:64] + out[64:]
            turned = jnp.concatenate([out[:, :LANES], out[:, LANES:]], axis=0).T
            for r in range(4):
                row = part * 32 + k * 4 + r
                out_ref[pl.ds(row, 32, stride=72), :] = turned[r * 32 : (r + 1) * 32]
    first = jnp.concatenate([first_ref[...], jnp.zeros((8, LANES - 16), jnp.float32)], axis=1)
    for k in range(8):
        out_ref[pl.ds(64 + k, 32, stride=72), :] = jnp.broadcast_to(first[k : k + 1], (32, LANES))


def spectrum_chunks(spec, factor, first):
    return pl.pallas_call(
        spectrum_kernel,
        out_shape=jax.ShapeDtypeStruct((32 * 72, LANES), jnp.float32),
        compiler_params=pltpu.CompilerParams(vmem_limit_bytes=VMEM_SMALL),
        name="spectrum_chunks",
    )(spec, factor, first)


def mode_kernel(core_ref, spec_ref, out_ref, w_ref, x_ref, v_ref):
    of_s = iota((128, 16), 0) >> 3 == iota((128, 16), 1)
    of_k = (iota((LANES, 256), 1) >> 2) & 31 == iota((LANES, 256), 0)
    row, col = iota((128, 256), 0), iota((128, 256), 1)
    same = (((row >> 2) & 1) == (col >> 7)) & ((row & 3) == (col & 3))
    first = [spec_ref[a, 0, 64:72, :] for a in range(4)]
    first = jnp.concatenate(first + [jnp.zeros((96, LANES), jnp.float32)], axis=0)
    first = pick_lanes(first.T[:16], of_k)
    expand = jnp.where(same, pick(of_s, first), 0.0)
    high, low = split(expand)
    expand_high = jnp.concatenate([high, high], axis=0)
    expand_low = jnp.concatenate([low, low], axis=0)

    for src in range(8):
        for pair in range(4):
            block = core_ref[:, src, :, pair * LANES : (pair + 1) * LANES].reshape(128, LANES)
            turned = jnp.concatenate(split(block.T), axis=1)
            w = dot(turned, expand_high) + dot(turned, expand_low)
            for half in range(2):
                rows = w[half * 64 : (half + 1) * 64]
                p = src * 8 + pair * 2 + half
                w_ref[p, 0] = rows[:, :LANES]
                w_ref[p, 1] = rows[:, LANES:]
                w_ref[p, 2] = rows[:, :LANES] + rows[:, LANES:]

    for src in range(8):
        parts = [
            spec_ref[:, src, part * 32 : (part + 1) * 32, :].reshape(128, LANES).T
            for part in range(2)
        ]
        parts.append(parts[0] + parts[1])
        for part in range(3):
            for b in range(2):
                x_ref[src * 2 + b, part] = parts[part][b * 64 : (b + 1) * 64]

    @pl.loop(0, 16)
    def _(step):
        samples, q0 = step // 4 * 4, pl.multiple_of(step % 4 * 16, 16)

        def one(p, sums):
            w = [w_ref[p, part, pl.ds(q0, 16), :] for part in range(3)]
            return tuple(
                sums[b * 3 + part] + x_ref[samples + b, part, pl.ds(p, 1), :] * w[part]
                for b in range(4)
                for part in range(3)
            )

        zero = jnp.zeros((16, LANES), jnp.float32)
        sums = lax.fori_loop(0, 64, one, (zero,) * 12, unroll=8)
        for b in range(4):
            rr, ii, mixed = sums[b * 3 : b * 3 + 3]
            v_ref[samples + b, 0, pl.ds(q0, 16), :] = rr - ii
            v_ref[samples + b, 1, pl.ds(q0, 16), :] = mixed - rr - ii

    for src in range(8):
        for part in range(2):
            both = jnp.concatenate([v_ref[src * 2, part], v_ref[src * 2 + 1, part]], axis=0)
            out_ref[:, src, :, part * LANES : (part + 1) * LANES] = both.T.reshape(4, 32, LANES)


def mode_products(core, spec):
    return pl.pallas_call(
        mode_kernel,
        out_shape=jax.ShapeDtypeStruct((4, 8, 32, 256), jnp.float32),
        scratch_shapes=[
            pltpu.VMEM((64, 3, 64, LANES), jnp.float32),
            pltpu.VMEM((16, 3, 64, LANES), jnp.float32),
            pltpu.VMEM((16, 2, 64, LANES), jnp.float32),
        ],
        compiler_params=pltpu.CompilerParams(vmem_limit_bytes=VMEM_LARGE),
        name="mode_products",
    )(core, spec)


def output_kernel(value_ref, factor_ref, out_ref):
    high, low = split(factor_ref[...].T)
    factor = jnp.concatenate([high, high, low, low], axis=1)
    for k in range(8):
        rows = [value_ref[pl.ds(k * 4 + r, 32, stride=32), :] for r in range(4)]
        turned = jnp.concatenate(rows, axis=0).T
        turned = jnp.concatenate([turned[:64], turned[64:]], axis=1)
        high, low = split(turned)
        out = dot(factor, jnp.concatenate([high, low, high, low], axis=0))
        for b in range(2):
            out_ref[0, b, pl.ds(k, 128, stride=8), :] = out[:, b * LANES : (b + 1) * LANES]


def output_modes(values, factor):
    return pl.pallas_call(
        output_kernel,
        grid=(2,),
        in_specs=[
            pl.BlockSpec((1024, LANES), lambda i: (0, i)),
            pl.BlockSpec((64, 128), lambda i: (0, 0)),
        ],
        out_specs=pl.BlockSpec((1, 2, 1024, LANES), lambda i: (i, 0, 0, 0)),
        out_shape=jax.ShapeDtypeStruct((2, 2, 1024, LANES), jnp.float32),
        compiler_params=pltpu.CompilerParams(vmem_limit_bytes=VMEM_SMALL),
        name="output_modes",
    )(values, factor)


def swap(chunks, axes):
    return lax.all_to_all(chunks, axes, split_axis=0, concat_axis=0, tiled=True)


def per_device(
    spectrum, core_tensor, input_factor, output_factor, first_factor, second_factor, third_factor
):
    second = lax.all_gather(second_factor, "my", axis=0, tiled=True)
    core = jnp.transpose(core_tensor, (0, 1, 3, 4, 5, 2)).reshape(2, 8, 256, 64)
    core = core_chunks(core, second, third_factor)
    core = swap(core.reshape(128, 8, 512), ("mx", "my", "col"))
    spec = spectrum_chunks(spectrum.reshape(2, 2, 1024, LANES), input_factor.T, first_factor)
    spec = swap(spec.reshape(32, 72, LANES), ("mx", "col"))
    values = mode_products(core.reshape(16, 8, 8, 512), spec.reshape(4, 8, 72, LANES))
    values = swap(values.reshape(32, 32, 256), ("mx", "col"))
    out = output_modes(values.reshape(1024, 256), output_factor.T)
    return out.reshape(spectrum.shape)


def solution(mesh):
    placed = (
        P(None, "col", None, "mx", "my"),
        P(None, "col", None, ("mx", "my"), None, None),
        P(),
        P(),
        P("mx", None),
        P("my", None),
        P(),
    )
    return jax.shard_map(
        per_device,
        mesh=mesh,
        in_specs=placed,
        out_specs=P(None, "col", None, "mx", "my"),
        check_vma=False,
    )
```

```python
import jax
import jax.numpy as jnp
from jax import lax
from jax.experimental import pallas as pl
from jax.experimental.pallas import tpu as pltpu
from jax.sharding import PartitionSpec as P

LANES = 128
CHUNK = 48
VMEM_SMALL = 16 * 2**20
VMEM_LARGE = 32 * 2**20


def dot(a, b):
    return jnp.dot(a, b, preferred_element_type=jnp.float32)


def split(x):
    high = x.astype(jnp.bfloat16)
    return high, (x - high.astype(jnp.float32)).astype(jnp.bfloat16)


def split3(x):
    high = x.astype(jnp.bfloat16)
    return (high, *split(x - high.astype(jnp.float32)))


def iota(shape, dim):
    return lax.broadcasted_iota(jnp.int32, shape, dim)


def pick(chosen, table):
    one = chosen.astype(jnp.bfloat16)
    high, mid, low = split3(table)
    return (dot(one, high) + dot(one, mid)) + dot(one, low)


def pick_lanes(table, chosen):
    one = chosen.astype(jnp.bfloat16)
    high, mid, low = split3(table)
    return (dot(high, one) + dot(mid, one)) + dot(low, one)


def send_kernel(spec_ref, core_ref, in_ref, factors_ref, third_ref, out_ref):
    high, low = split(in_ref[...])
    rows = jnp.concatenate(
        [jnp.concatenate([high, high], axis=1), jnp.concatenate([low, low], axis=1)], axis=0
    )
    for b in range(2):
        for k in range(8):
            both = jnp.concatenate(
                [spec_ref[part, b, pl.ds(k, 128, stride=8), :] for part in range(2)], axis=1
            )
            out = dot(rows, jnp.concatenate(split(both), axis=0))
            out = out[:64] + out[64:]
            turned = jnp.concatenate([out[:, :LANES], out[:, LANES:]], axis=0).T
            out_ref[pl.ds(2 * k + b, 128, stride=CHUNK), :] = turned

    of_t = iota((16, 256), 1) >> 4 == iota((16, 256), 0)
    of_u = iota((16, 256), 1) & 15 == iota((16, 256), 0)
    second = pick_lanes(factors_ref[:32, 16:32], of_t)
    third = pick_lanes(third_ref[...], of_u)
    by_y = pick(iota((512, 32), 0) >> 4 == iota((512, 32), 1), second)
    by_z = pick(iota((512, 16), 0) & 15 == iota((512, 16), 1), third)
    mat_high, mat_low = split(by_y * by_z)
    for pair in range(4):
        both = jnp.concatenate(
            [core_ref[part, 2 * pair + half] for half in range(2) for part in range(2)], axis=1
        )
        high, low = split(both)
        out = dot(mat_high, high) + dot(mat_high, low) + dot(mat_low, high)
        for half in range(2):
            for r in range(4):
                row = 16 + (2 * pair + half) * 4 + r
                out_ref[pl.ds(row, 128, stride=CHUNK), :] = out[
                    r * 128 : (r + 1) * 128, half * LANES : (half + 1) * LANES
                ]


def send_chunks(spec, core, factor, factors, third):
    return pl.pallas_call(
        send_kernel,
        out_shape=jax.ShapeDtypeStruct((128 * CHUNK, LANES), jnp.float32),
        compiler_params=pltpu.CompilerParams(vmem_limit_bytes=VMEM_SMALL),
        name="send_chunks",
    )(spec, core, factor, factors, third)


def mode_kernel(got_ref, factors_ref, out_ref, w_ref):
    of_s = iota((16, 128), 1) >> 3 == iota((16, 128), 0)
    row, col = iota((256, 128), 0), iota((256, 128), 1)
    of_k = ((row >> 5) & 3) * 32 + (row & 7) == col
    same = ((row >> 7) == ((col >> 2) & 1)) & (((row >> 3) & 3) == (col & 3))
    first = pick_lanes(factors_ref[:, :16], of_s)
    high, low = split(jnp.where(same, pick(of_k, first), 0.0))
    expand = jnp.concatenate(
        [jnp.concatenate([high, high], axis=1), jnp.concatenate([low, low], axis=1)], axis=0
    )
    for src in range(8):
        for two in range(2):
            blocks = [
                got_ref[:, src, 16 + 8 * pair : 24 + 8 * pair, :].reshape(128, LANES)
                for pair in (2 * two, 2 * two + 1)
            ]
            out = dot(expand, jnp.concatenate(split(jnp.concatenate(blocks, axis=1)), axis=0))
            out = out[:256] + out[256:]
            for pair in range(2):
                for half in range(2):
                    p = src * 8 + (2 * two + pair) * 2 + half
                    w_ref[pl.ds(p, 128, stride=64), :] = out[
                        half * 128 : (half + 1) * 128, pair * LANES : (pair + 1) * LANES
                    ]

    got = got_ref.reshape(128 * CHUNK, LANES)
    left = iota((16, LANES), 1) < 64

    @pl.loop(0, 16)
    def _(g):
        for k in range(8):
            x = jnp.concatenate(
                [got[pl.ds(g * 8 * CHUNK + 2 * k + b, 8, stride=CHUNK), :] for b in range(2)],
                axis=0,
            )
            swapped = pltpu.roll(x, 64, 1)
            real, imag = jnp.where(left, x, swapped), jnp.where(left, swapped, x)
            rows = jnp.concatenate([*split(real), *split(imag)], axis=0)
            w = w_ref[pl.ds(pl.multiple_of((g * 8 + k) * 64, 64), 64), :]
            out = dot(rows, jnp.concatenate(split(w), axis=0))
            by_real, by_imag = out[:16] + out[16:32], out[32:48] + out[48:]
            swapped = pltpu.roll(by_imag, 64, 1)
            value = by_real + jnp.where(left, -swapped, swapped)
            for b in range(2):
                out_ref[pl.ds(g * 128 + 2 * k + b, 8, stride=16), :] = value[b * 8 : (b + 1) * 8]


def mode_products(got, factors):
    return pl.pallas_call(
        mode_kernel,
        out_shape=jax.ShapeDtypeStruct((128 * 16, LANES), jnp.float32),
        scratch_shapes=[pltpu.VMEM((128 * 64, LANES), jnp.float32)],
        compiler_params=pltpu.CompilerParams(vmem_limit_bytes=VMEM_LARGE),
        name="mode_products",
    )(got, factors)


def output_kernel(value_ref, factor_ref, out_ref):
    high, low = split(factor_ref[...].T)
    factor = jnp.concatenate([high, high, low, low], axis=1)
    step = pl.program_id(0)
    for k in range(8):
        turned = value_ref[pl.ds(2 * k + step, 128, stride=16), :].T
        high, low = split(jnp.concatenate([turned[:64], turned[64:]], axis=1))
        out = dot(factor, jnp.concatenate([high, low, high, low], axis=0))
        for part in range(2):
            out_ref[part, 0, pl.ds(k, 128, stride=8), :] = out[:, part * LANES : (part + 1) * LANES]


def output_modes(values, factor):
    return pl.pallas_call(
        output_kernel,
        grid=(2,),
        in_specs=[
            pl.BlockSpec((2048, LANES), lambda i: (0, 0)),
            pl.BlockSpec((64, 128), lambda i: (0, 0)),
        ],
        out_specs=pl.BlockSpec((2, 1, 1024, LANES), lambda i: (0, i, 0, 0)),
        out_shape=jax.ShapeDtypeStruct((2, 2, 1024, LANES), jnp.float32),
        compiler_params=pltpu.CompilerParams(vmem_limit_bytes=VMEM_SMALL),
        name="output_modes",
    )(values, factor)


def swap(chunks, axes):
    return lax.all_to_all(chunks, axes, split_axis=0, concat_axis=0, tiled=True)


def per_device(
    spectrum, core_tensor, input_factor, output_factor, first_factor, second_factor, third_factor
):
    mine = jnp.concatenate(
        [first_factor, second_factor, jnp.zeros((8, LANES - 32), jnp.float32)], axis=1
    )
    factors = swap(jnp.broadcast_to(mine, (16, 8, LANES)), ("mx", "my")).reshape(128, LANES)
    everyone = ("mx", "my", "col")
    core = jnp.transpose(core_tensor, (0, 1, 3, 4, 5, 2)).reshape(2, 8, 256, 64)
    chunks = send_chunks(
        spectrum.reshape(2, 2, 1024, LANES), core, input_factor.T, factors, third_factor
    )
    got = swap(chunks.reshape(128, CHUNK, LANES), everyone)
    values = mode_products(got.reshape(16, 8, CHUNK, LANES), factors)
    values = swap(values.reshape(128, 16, LANES), everyone)
    out = output_modes(values.reshape(2048, LANES), output_factor.T)
    return out.reshape(spectrum.shape)


def solution(mesh):
    placed = (
        P(None, "col", None, "mx", "my"),
        P(None, "col", None, ("mx", "my"), None, None),
        P(),
        P(),
        P("mx", None),
        P("my", None),
        P(),
    )
    return jax.shard_map(
        per_device,
        mesh=mesh,
        in_specs=placed,
        out_specs=P(None, "col", None, "mx", "my"),
        check_vma=False,
    )
```

```python
import jax
import jax.numpy as jnp
from jax import lax
from jax.experimental import pallas as pl
from jax.experimental.pallas import tpu as pltpu
from jax.sharding import PartitionSpec as P

LANES = 128
CHUNK = 49
WIDE = 72
VMEM_SMALL = 16 * 2**20
VMEM_ALONE = 56 * 2**20
VMEM_LARGE = 32 * 2**20


def dot(a, b):
    return jnp.dot(a, b, preferred_element_type=jnp.float32)


def split(x):
    high = x.astype(jnp.bfloat16)
    return high, (x - high.astype(jnp.float32)).astype(jnp.bfloat16)


def split3(x):
    high = x.astype(jnp.bfloat16)
    return (high, *split(x - high.astype(jnp.float32)))


def iota(shape, dim):
    return lax.broadcasted_iota(jnp.int32, shape, dim)


def pick(chosen, table):
    one = chosen.astype(jnp.bfloat16)
    high, mid, low = split3(table)
    return (dot(one, high) + dot(one, mid)) + dot(one, low)


def pick_lanes(table, chosen):
    one = chosen.astype(jnp.bfloat16)
    high, mid, low = split3(table)
    return (dot(high, one) + dot(mid, one)) + dot(low, one)


def send_kernel(
    spec_hbm, core_hbm, in_ref, first_ref, second_ref, third_ref, out_ref, spec_ref, core_ref, sems
):
    def spec_copy(b):
        return pltpu.make_async_copy(spec_hbm.at[:, b], spec_ref.at[:, b], sems.at[b])

    def core_copy(pair):
        some = pl.ds(2 * pair, 2)
        return pltpu.make_async_copy(core_hbm.at[:, some], core_ref.at[:, some], sems.at[2 + pair])

    for b in range(2):
        spec_copy(b).start()
    for pair in range(4):
        core_copy(pair).start()

    of_s = iota((16, 128), 1) & 15 == iota((16, 128), 0)
    mine = pick_lanes(first_ref[...], of_s)
    mine = jnp.where(iota((8, 128), 1) >> 4 == iota((8, 128), 0), mine, 0.0)
    mine = jnp.sum(mine, axis=0, keepdims=True)
    out_ref[pl.ds(48, 128, stride=CHUNK), :] = jnp.broadcast_to(mine, (128, LANES))

    high, low = split(in_ref[...])
    rows = jnp.concatenate(
        [jnp.concatenate([high, high], axis=1), jnp.concatenate([low, low], axis=1)], axis=0
    )
    for b in range(2):
        spec_copy(b).wait()
        for k in range(8):
            both = jnp.concatenate(
                [spec_ref[part, b, pl.ds(k, 128, stride=8), :] for part in range(2)], axis=1
            )
            out = dot(rows, jnp.concatenate(split(both), axis=0))
            out = out[:64] + out[64:]
            turned = jnp.concatenate([out[:, :LANES], out[:, LANES:]], axis=0).T
            out_ref[pl.ds(2 * k + b, 128, stride=CHUNK), :] = turned

    of_t = iota((16, 256), 1) >> 4 == iota((16, 256), 0)
    of_u = iota((16, 256), 1) & 15 == iota((16, 256), 0)
    second = pick_lanes(second_ref[...], of_t)
    third = pick_lanes(third_ref[...], of_u)
    by_y = pick(iota((512, 32), 0) >> 4 == iota((512, 32), 1), second)
    by_z = pick(iota((512, 16), 0) & 15 == iota((512, 16), 1), third)
    mat_high, mat_low = split(by_y * by_z)
    for pair in range(4):
        if pair % 2 == 0:
            core_copy(pair).wait()
            core_copy(pair + 1).wait()
        both = jnp.concatenate(
            [core_ref[part, 2 * pair + half] for half in range(2) for part in range(2)], axis=1
        )
        high, low = split(both)
        out = dot(mat_high, high) + dot(mat_high, low) + dot(mat_low, high)
        for half in range(2):
            for r in range(4):
                row = 16 + (2 * pair + half) * 4 + r
                out_ref[pl.ds(row, 128, stride=CHUNK), :] = out[
                    r * 128 : (r + 1) * 128, half * LANES : (half + 1) * LANES
                ]


def send_chunks(spec, core, *factors):
    whole = pl.BlockSpec(memory_space=pltpu.VMEM)
    return pl.pallas_call(
        send_kernel,
        in_specs=[pl.BlockSpec(memory_space=pl.ANY)] * 2 + [whole] * 4,
        out_shape=jax.ShapeDtypeStruct((128 * CHUNK, LANES), jnp.float32),
        scratch_shapes=[
            pltpu.VMEM(spec.shape, jnp.float32),
            pltpu.VMEM(core.shape, jnp.float32),
            pltpu.SemaphoreType.DMA((6,)),
        ],
        compiler_params=pltpu.CompilerParams(vmem_limit_bytes=VMEM_ALONE),
        name="send_chunks",
    )(spec, core, *factors)


def mode_kernel(got, out_ref, w_ref):
    row, col = iota((256, 128), 0), iota((256, 128), 1)
    first = jnp.concatenate([got[pl.ds(a * 32 * CHUNK + 48, 1), :] for a in range(4)] * 2, axis=0)
    first = pick((iota((256, 8), 0) >> 5) & 3 == iota((256, 8), 1), first)
    first = jnp.where(col >> 4 == row & 7, first, 0.0)
    first = pick_lanes(first, iota((128, 128), 0) & 15 == iota((128, 128), 1) >> 3)
    same = ((row >> 7) == ((col >> 2) & 1)) & (((row >> 3) & 3) == (col & 3))
    high, low = split(jnp.where(same, first, 0.0))
    expand = jnp.concatenate(
        [jnp.concatenate([high, high], axis=1), jnp.concatenate([low, low], axis=1)], axis=0
    )

    @pl.loop(0, 8)
    def _(src):
        for two in range(2):
            blocks = [
                jnp.concatenate(
                    [
                        got[pl.ds((s * 8 + src) * CHUNK + 16 + 8 * pair, 8), :]
                        for s in range(16)
                    ],
                    axis=0,
                )
                for pair in (2 * two, 2 * two + 1)
            ]
            out = dot(expand, jnp.concatenate(split(jnp.concatenate(blocks, axis=1)), axis=0))
            out = out[:256] + out[256:]
            for pair in range(2):
                for half in range(2):
                    p = src * 8 + (2 * two + pair) * 2 + half
                    w_ref[pl.ds(p, 128, stride=WIDE), :] = out[
                        half * 128 : (half + 1) * 128, pair * LANES : (pair + 1) * LANES
                    ]

    left = iota((16, LANES), 1) < 64

    @pl.loop(0, 16)
    def _(g):
        for k in range(8):
            x = jnp.concatenate(
                [got[pl.ds(g * 8 * CHUNK + 2 * k + b, 8, stride=CHUNK), :] for b in range(2)],
                axis=0,
            )
            swapped = pltpu.roll(x, 64, 1)
            real, imag = jnp.where(left, x, swapped), jnp.where(left, swapped, x)
            rows = jnp.concatenate([*split(real), *split(imag)], axis=0)
            w = w_ref[pl.ds(pl.multiple_of((g * 8 + k) * WIDE, 8), 64), :]
            out = dot(rows, jnp.concatenate(split(w), axis=0))
            by_real, by_imag = out[:16] + out[16:32], out[32:48] + out[48:]
            swapped = pltpu.roll(by_imag, 64, 1)
            value = by_real + jnp.where(left, -swapped, swapped)
            for b in range(2):
                out_ref[pl.ds(g * 128 + 2 * k + b, 8, stride=16), :] = value[b * 8 : (b + 1) * 8]


def mode_products(got):
    return pl.pallas_call(
        mode_kernel,
        out_shape=jax.ShapeDtypeStruct((128 * 16, LANES), jnp.float32),
        scratch_shapes=[pltpu.VMEM((128 * WIDE, LANES), jnp.float32)],
        compiler_params=pltpu.CompilerParams(vmem_limit_bytes=VMEM_LARGE),
        name="mode_products",
    )(got)


def output_kernel(value_ref, factor_ref, out_ref):
    high, low = split(factor_ref[...].T)
    factor = jnp.concatenate([high, high, low, low], axis=1)
    step = pl.program_id(0)
    for k in range(8):
        turned = value_ref[pl.ds(2 * k + step, 128, stride=16), :].T
        high, low = split(jnp.concatenate([turned[:64], turned[64:]], axis=1))
        out = dot(factor, jnp.concatenate([high, low, high, low], axis=0))
        for part in range(2):
            out_ref[part, 0, pl.ds(k, 128, stride=8), :] = out[:, part * LANES : (part + 1) * LANES]


def output_modes(values, factor):
    return pl.pallas_call(
        output_kernel,
        grid=(2,),
        in_specs=[
            pl.BlockSpec((2048, LANES), lambda i: (0, 0)),
            pl.BlockSpec((64, 128), lambda i: (0, 0)),
        ],
        out_specs=pl.BlockSpec((2, 1, 1024, LANES), lambda i: (0, i, 0, 0)),
        out_shape=jax.ShapeDtypeStruct((2, 2, 1024, LANES), jnp.float32),
        compiler_params=pltpu.CompilerParams(vmem_limit_bytes=VMEM_SMALL),
        name="output_modes",
    )(values, factor)


def swap(chunks, axes):
    return lax.all_to_all(chunks, axes, split_axis=0, concat_axis=0, tiled=True)


def per_device(
    spectrum, core_tensor, input_factor, output_factor, first_factor, second_factor, third_factor
):
    everyone = ("mx", "my", "col")
    second = lax.all_gather(second_factor, "my", axis=0, tiled=True)
    core = jnp.transpose(core_tensor, (0, 1, 3, 4, 5, 2)).reshape(2, 8, 256, 64)
    spec = spectrum.reshape(2, 2, 1024, LANES)
    chunks = send_chunks(spec, core, input_factor.T, first_factor, second, third_factor)
    got = swap(chunks.reshape(128, 1, CHUNK * LANES), everyone)
    values = mode_products(got.reshape(128 * CHUNK, LANES))
    values = swap(values.reshape(128, 16, LANES), everyone)
    out = output_modes(values.reshape(2048, LANES), output_factor.T)
    return out.reshape(spectrum.shape)


def solution(mesh):
    placed = (
        P(None, "col", None, "mx", "my"),
        P(None, "col", None, ("mx", "my"), None, None),
        P(),
        P(),
        P("mx", None),
        P("my", None),
        P(),
    )
    return jax.shard_map(
        per_device,
        mesh=mesh,
        in_specs=placed,
        out_specs=P(None, "col", None, "mx", "my"),
        check_vma=False,
    )
```

```python
import jax
import jax.numpy as jnp
from jax import lax
from jax.experimental import pallas as pl
from jax.experimental.pallas import tpu as pltpu
from jax.sharding import PartitionSpec as P

LANES = 128
CHUNK = 49
WIDE = 72
VMEM_SMALL = 16 * 2**20
VMEM_ALONE = 56 * 2**20
VMEM_LARGE = 32 * 2**20


def dot(a, b):
    return jnp.dot(a, b, preferred_element_type=jnp.float32)


def split(x):
    high = x.astype(jnp.bfloat16)
    return high, (x - high.astype(jnp.float32)).astype(jnp.bfloat16)


def split3(x):
    high = x.astype(jnp.bfloat16)
    return (high, *split(x - high.astype(jnp.float32)))


def iota(shape, dim):
    return lax.broadcasted_iota(jnp.int32, shape, dim)


def pick(chosen, table):
    one = chosen.astype(jnp.bfloat16)
    high, mid, low = split3(table)
    return (dot(one, high) + dot(one, mid)) + dot(one, low)


def pick_lanes(table, chosen):
    one = chosen.astype(jnp.bfloat16)
    high, mid, low = split3(table)
    return (dot(high, one) + dot(mid, one)) + dot(low, one)


def send_kernel(
    spec_hbm, core_hbm, in_ref, first_ref, second_ref, third_ref, out_ref, spec_ref, core_ref, sems
):
    def spec_copy(b):
        return pltpu.make_async_copy(spec_hbm.at[:, b], spec_ref.at[:, b], sems.at[b])

    def core_copy(pair):
        some = pl.ds(2 * pair, 2)
        return pltpu.make_async_copy(core_hbm.at[:, some], core_ref.at[:, some], sems.at[2 + pair])

    for b in range(2):
        spec_copy(b).start()
    for pair in range(4):
        core_copy(pair).start()

    of_s = iota((16, 128), 1) & 15 == iota((16, 128), 0)
    mine = pick_lanes(first_ref[...], of_s)
    mine = jnp.where(iota((8, 128), 1) >> 4 == iota((8, 128), 0), mine, 0.0)
    mine = jnp.sum(mine, axis=0, keepdims=True)
    out_ref[pl.ds(48, 128, stride=CHUNK), :] = jnp.broadcast_to(mine, (128, LANES))

    of_t = iota((16, 256), 1) >> 4 == iota((16, 256), 0)
    of_u = iota((16, 256), 1) & 15 == iota((16, 256), 0)
    second = pick_lanes(second_ref[...], of_t)
    third = pick_lanes(third_ref[...], of_u)
    by_y = pick(iota((512, 32), 0) >> 4 == iota((512, 32), 1), second)
    by_z = pick(iota((512, 16), 0) & 15 == iota((512, 16), 1), third)
    mat_high, mat_low = split(by_y * by_z)

    high, low = split(in_ref[...])
    rows = jnp.concatenate(
        [jnp.concatenate([high, high], axis=1), jnp.concatenate([low, low], axis=1)], axis=0
    )
    for b in range(2):
        spec_copy(b).wait()
    for b in range(2):
        for k in range(8):
            both = jnp.concatenate(
                [spec_ref[part, b, pl.ds(k, 128, stride=8), :] for part in range(2)], axis=1
            )
            out = dot(rows, jnp.concatenate(split(both), axis=0))
            out = out[:64] + out[64:]
            turned = jnp.concatenate([out[:, :LANES], out[:, LANES:]], axis=0).T
            out_ref[pl.ds(2 * k + b, 128, stride=CHUNK), :] = turned

    for pair in range(4):
        core_copy(pair).wait()
    for pair in range(4):
        both = jnp.concatenate(
            [core_ref[part, 2 * pair + half] for half in range(2) for part in range(2)], axis=1
        )
        high, low = split(both)
        out = dot(mat_high, high) + dot(mat_high, low) + dot(mat_low, high)
        for half in range(2):
            for r in range(4):
                row = 16 + (2 * pair + half) * 4 + r
                out_ref[pl.ds(row, 128, stride=CHUNK), :] = out[
                    r * 128 : (r + 1) * 128, half * LANES : (half + 1) * LANES
                ]


def send_chunks(spec, core, *factors):
    whole = pl.BlockSpec(memory_space=pltpu.VMEM)
    return pl.pallas_call(
        send_kernel,
        in_specs=[pl.BlockSpec(memory_space=pl.ANY)] * 2 + [whole] * 4,
        out_shape=pltpu.VMEM((128 * CHUNK, LANES), jnp.float32),
        scratch_shapes=[
            pltpu.VMEM(spec.shape, jnp.float32),
            pltpu.VMEM(core.shape, jnp.float32),
            pltpu.SemaphoreType.DMA((6,)),
        ],
        compiler_params=pltpu.CompilerParams(vmem_limit_bytes=VMEM_ALONE),
        name="send_chunks",
    )(spec, core, *factors)


def mode_kernel(got, out_ref, w_ref):
    row, col = iota((256, 128), 0), iota((256, 128), 1)
    first = jnp.concatenate([got[pl.ds(a * 32 * CHUNK + 48, 1), :] for a in range(4)] * 2, axis=0)
    first = pick((iota((256, 8), 0) >> 5) & 3 == iota((256, 8), 1), first)
    first = jnp.where(col >> 4 == row & 7, first, 0.0)
    first = pick_lanes(first, iota((128, 128), 0) & 15 == iota((128, 128), 1) >> 3)
    same = ((row >> 7) == ((col >> 2) & 1)) & (((row >> 3) & 3) == (col & 3))
    high, low = split(jnp.where(same, first, 0.0))
    expand = jnp.concatenate(
        [jnp.concatenate([high, high], axis=1), jnp.concatenate([low, low], axis=1)], axis=0
    )

    for src in range(8):
        for two in range(2):
            blocks = [
                jnp.concatenate(
                    [
                        got[pl.ds((s * 8 + src) * CHUNK + 16 + 8 * pair, 8), :]
                        for s in range(16)
                    ],
                    axis=0,
                )
                for pair in (2 * two, 2 * two + 1)
            ]
            out = dot(expand, jnp.concatenate(split(jnp.concatenate(blocks, axis=1)), axis=0))
            out = out[:256] + out[256:]
            for pair in range(2):
                for half in range(2):
                    p = src * 8 + (2 * two + pair) * 2 + half
                    w_ref[pl.ds(p, 128, stride=WIDE), :] = out[
                        half * 128 : (half + 1) * 128, pair * LANES : (pair + 1) * LANES
                    ]

    left = iota((16, LANES), 1) < 64

    for g in range(16):
        for k in range(8):
            x = jnp.concatenate(
                [got[pl.ds(g * 8 * CHUNK + 2 * k + b, 8, stride=CHUNK), :] for b in range(2)],
                axis=0,
            )
            swapped = pltpu.roll(x, 64, 1)
            real, imag = jnp.where(left, x, swapped), jnp.where(left, swapped, x)
            rows = jnp.concatenate([*split(real), *split(imag)], axis=0)
            w = w_ref[pl.ds((g * 8 + k) * WIDE, 64), :]
            out = dot(rows, jnp.concatenate(split(w), axis=0))
            by_real, by_imag = out[:16] + out[16:32], out[32:48] + out[48:]
            swapped = pltpu.roll(by_imag, 64, 1)
            value = by_real + jnp.where(left, -swapped, swapped)
            for b in range(2):
                out_ref[pl.ds(g * 128 + 2 * k + b, 8, stride=16), :] = value[b * 8 : (b + 1) * 8]


def mode_products(got):
    return pl.pallas_call(
        mode_kernel,
        out_shape=jax.ShapeDtypeStruct((128 * 16, LANES), jnp.float32),
        scratch_shapes=[pltpu.VMEM((128 * WIDE, LANES), jnp.float32)],
        compiler_params=pltpu.CompilerParams(vmem_limit_bytes=VMEM_LARGE),
        name="mode_products",
    )(got)


def output_kernel(value_ref, factor_ref, out_ref):
    high, low = split(factor_ref[...].T)
    factor = jnp.concatenate([high, high, low, low], axis=1)
    step = pl.program_id(0)
    for k in range(8):
        turned = value_ref[pl.ds(2 * k + step, 128, stride=16), :].T
        high, low = split(jnp.concatenate([turned[:64], turned[64:]], axis=1))
        out = dot(factor, jnp.concatenate([high, low, high, low], axis=0))
        for part in range(2):
            out_ref[part, 0, pl.ds(k, 128, stride=8), :] = out[:, part * LANES : (part + 1) * LANES]


def output_modes(values, factor):
    return pl.pallas_call(
        output_kernel,
        grid=(2,),
        in_specs=[
            pl.BlockSpec((2048, LANES), lambda i: (0, 0)),
            pl.BlockSpec((64, 128), lambda i: (0, 0)),
        ],
        out_specs=pl.BlockSpec((2, 1, 1024, LANES), lambda i: (0, i, 0, 0)),
        out_shape=jax.ShapeDtypeStruct((2, 2, 1024, LANES), jnp.float32),
        compiler_params=pltpu.CompilerParams(vmem_limit_bytes=VMEM_SMALL),
        name="output_modes",
    )(values, factor)


def swap(chunks, axes):
    return lax.all_to_all(chunks, axes, split_axis=0, concat_axis=0, tiled=True)


def per_device(
    spectrum, core_tensor, input_factor, output_factor, first_factor, second_factor, third_factor
):
    everyone = ("mx", "my", "col")
    second = lax.all_gather(second_factor, "my", axis=0, tiled=True)
    core = jnp.transpose(core_tensor, (0, 1, 3, 4, 5, 2)).reshape(2, 8, 256, 64)
    spec = spectrum.reshape(2, 2, 1024, LANES)
    chunks = send_chunks(spec, core, input_factor.T, first_factor, second, third_factor)
    got = swap(chunks.reshape(128, 1, CHUNK * LANES), everyone)
    values = mode_products(got.reshape(128 * CHUNK, LANES))
    values = swap(values.reshape(128, 16, LANES), everyone)
    out = output_modes(values.reshape(2048, LANES), output_factor.T)
    return out.reshape(spectrum.shape)


def solution(mesh):
    placed = (
        P(None, "col", None, "mx", "my"),
        P(None, "col", None, ("mx", "my"), None, None),
        P(),
        P(),
        P("mx", None),
        P("my", None),
        P(),
    )
    return jax.shard_map(
        per_device,
        mesh=mesh,
        in_specs=placed,
        out_specs=P(None, "col", None, "mx", "my"),
        check_vma=False,
    )
```

```python
import jax
import jax.numpy as jnp
from jax import lax
from jax.experimental import pallas as pl
from jax.experimental.pallas import tpu as pltpu
from jax.sharding import PartitionSpec as P


LANES = 128
CHUNK = 49
WIDE = 72
VMEM_SMALL = 16 * 2**20
VMEM_ALONE = 56 * 2**20
VMEM_LARGE = 32 * 2**20


def dot(a, b):
    return jnp.dot(a, b, preferred_element_type=jnp.float32)


def split(x):
    high = x.astype(jnp.bfloat16)
    return high, (x - high.astype(jnp.float32)).astype(jnp.bfloat16)


def split3(x):
    high = x.astype(jnp.bfloat16)
    return (high, *split(x - high.astype(jnp.float32)))


def iota(shape, dim):
    return lax.broadcasted_iota(jnp.int32, shape, dim)


def pick(chosen, table):
    one = chosen.astype(jnp.bfloat16)
    high, mid, low = split3(table)
    return (dot(one, high) + dot(one, mid)) + dot(one, low)


def pick_lanes(table, chosen):
    one = chosen.astype(jnp.bfloat16)
    high, mid, low = split3(table)
    return (dot(high, one) + dot(mid, one)) + dot(low, one)


def spectrum_kernel(
    spec_hbm, core_hbm, in_hbm, first_hbm, out_ref, half_ref, spec_ref, core_ref, in_ref, first_ref, sems
):
    def copy(source, target, n):
        made = pltpu.make_async_copy(source, target, sems.at[n])
        made.start()
        return made

    small = [copy(first_hbm, first_ref, 0), copy(in_hbm, in_ref, 1)]
    parts = [copy(spec_hbm.at[:, b], spec_ref.at[:, b], 2 + b) for b in range(2)]
    parts.append(copy(core_hbm, core_ref, 4))

    for made in small:
        made.wait()
    of_s = iota((16, 128), 1) & 15 == iota((16, 128), 0)
    mine = pick_lanes(first_ref[...], of_s)
    mine = jnp.where(iota((8, 128), 1) >> 4 == iota((8, 128), 0), mine, 0.0)
    mine = jnp.sum(mine, axis=0, keepdims=True)
    out_ref[pl.ds(48, 128, stride=CHUNK), :] = jnp.broadcast_to(mine, (128, LANES))

    high, low = split(in_ref[...])
    rows = jnp.concatenate(
        [jnp.concatenate([high, high], axis=1), jnp.concatenate([low, low], axis=1)], axis=0
    )
    for made in parts:
        made.wait()
    for b in range(2):
        for k in range(8):
            both = jnp.concatenate(
                [spec_ref[part, b, pl.ds(k, 128, stride=8), :] for part in range(2)], axis=1
            )
            out = dot(rows, jnp.concatenate(split(both), axis=0))
            out = out[:64] + out[64:]
            turned = jnp.concatenate([out[:, :LANES], out[:, LANES:]], axis=0).T
            out_ref[pl.ds(2 * k + b, 128, stride=CHUNK), :] = turned
    for pair in range(4):
        both = jnp.concatenate(
            [core_ref[part, 2 * pair + half] for half in range(2) for part in range(2)], axis=1
        )
        half_ref[pair, 0], half_ref[pair, 1] = split(both)


def spectrum_chunks(spec, core, factor, first):
    return pl.pallas_call(
        spectrum_kernel,
        in_specs=[pl.BlockSpec(memory_space=pl.ANY)] * 4,
        out_shape=(
            pltpu.VMEM((128 * CHUNK, LANES), jnp.float32),
            pltpu.VMEM((4, 2, 256, 256), jnp.bfloat16),
        ),
        scratch_shapes=[
            pltpu.VMEM(spec.shape, jnp.float32),
            pltpu.VMEM(core.shape, jnp.float32),
            pltpu.VMEM(factor.shape, jnp.float32),
            pltpu.VMEM(first.shape, jnp.float32),
            pltpu.SemaphoreType.DMA((5,)),
        ],
        compiler_params=pltpu.CompilerParams(vmem_limit_bytes=VMEM_ALONE),
        name="spectrum_chunks",
    )(spec, core, factor, first)


def core_kernel(_, half_ref, s0_ref, s1_ref, s2_ref, s3_ref, third_ref, out_ref):
    b = lax.axis_index("my")
    seconds = jnp.concatenate([ref[...] for ref in (s0_ref, s1_ref, s2_ref, s3_ref)], axis=0)
    of_t = iota((16, 256), 1) >> 4 == iota((16, 256), 0)
    of_u = iota((16, 256), 1) & 15 == iota((16, 256), 0)
    second, third = pick_lanes(seconds, of_t), pick_lanes(third_ref[...], of_u)
    row = iota((512, 32), 0)
    by_y = pick(((row >> 7) ^ b) * 8 + ((row & 127) >> 4) == iota((512, 32), 1), second)
    by_z = pick(iota((512, 16), 0) & 15 == iota((512, 16), 1), third)
    mat_high, mat_low = split(by_y * by_z)
    for pair in range(4):
        high, low = half_ref[pair, 0], half_ref[pair, 1]
        out = dot(mat_high, high) + dot(mat_high, low) + dot(mat_low, high)
        for half in range(2):
            for r in range(4):
                row = 16 + (2 * pair + half) * 4 + r
                out_ref[pl.ds(row, 128, stride=CHUNK), :] = out[
                    r * 128 : (r + 1) * 128, half * LANES : (half + 1) * LANES
                ]


def core_chunks(chunks, halves, seconds, third):
    whole = pl.BlockSpec(memory_space=pltpu.VMEM)
    return pl.pallas_call(
        core_kernel,
        in_specs=[pl.BlockSpec(memory_space=pl.ANY)] + [whole] * 6,
        out_shape=pltpu.VMEM((128 * CHUNK, LANES), jnp.float32),
        input_output_aliases={0: 0},
        compiler_params=pltpu.CompilerParams(vmem_limit_bytes=VMEM_SMALL),
        name="core_chunks",
    )(chunks, halves, *seconds, third)


def mode_kernel(got, out_ref, w_ref):
    row, col = iota((256, 128), 0), iota((256, 128), 1)
    first = jnp.concatenate([got[pl.ds(a * 32 * CHUNK + 48, 1), :] for a in range(4)] * 2, axis=0)
    first = pick((iota((256, 8), 0) >> 5) & 3 == iota((256, 8), 1), first)
    first = jnp.where(col >> 4 == row & 7, first, 0.0)
    first = pick_lanes(first, iota((128, 128), 0) & 15 == iota((128, 128), 1) >> 3)
    same = ((row >> 7) == ((col >> 2) & 1)) & (((row >> 3) & 3) == (col & 3))
    high, low = split(jnp.where(same, first, 0.0))
    expand = jnp.concatenate(
        [jnp.concatenate([high, high], axis=1), jnp.concatenate([low, low], axis=1)], axis=0
    )

    for src in range(8):
        for two in range(2):
            blocks = [
                jnp.concatenate(
                    [
                        got[pl.ds((s * 8 + src) * CHUNK + 16 + 8 * pair, 8), :]
                        for s in range(16)
                    ],
                    axis=0,
                )
                for pair in (2 * two, 2 * two + 1)
            ]
            out = dot(expand, jnp.concatenate(split(jnp.concatenate(blocks, axis=1)), axis=0))
            out = out[:256] + out[256:]
            for pair in range(2):
                for half in range(2):
                    p = src * 8 + (2 * two + pair) * 2 + half
                    w_ref[pl.ds(p, 128, stride=WIDE), :] = out[
                        half * 128 : (half + 1) * 128, pair * LANES : (pair + 1) * LANES
                    ]

    left = iota((16, LANES), 1) < 64

    for g in range(16):
        for k in range(8):
            x = jnp.concatenate(
                [got[pl.ds(g * 8 * CHUNK + 2 * k + b, 8, stride=CHUNK), :] for b in range(2)],
                axis=0,
            )
            swapped = pltpu.roll(x, 64, 1)
            real, imag = jnp.where(left, x, swapped), jnp.where(left, swapped, x)
            rows = jnp.concatenate([*split(real), *split(imag)], axis=0)
            w = w_ref[pl.ds((g * 8 + k) * WIDE, 64), :]
            out = dot(rows, jnp.concatenate(split(w), axis=0))
            by_real, by_imag = out[:16] + out[16:32], out[32:48] + out[48:]
            swapped = pltpu.roll(by_imag, 64, 1)
            value = by_real + jnp.where(left, -swapped, swapped)
            for b in range(2):
                out_ref[pl.ds(g * 128 + 2 * k + b, 8, stride=16), :] = value[b * 8 : (b + 1) * 8]


def mode_products(got):
    return pl.pallas_call(
        mode_kernel,
        out_shape=jax.ShapeDtypeStruct((128 * 16, LANES), jnp.float32),
        scratch_shapes=[pltpu.VMEM((128 * WIDE, LANES), jnp.float32)],
        compiler_params=pltpu.CompilerParams(vmem_limit_bytes=VMEM_LARGE),
        name="mode_products",
    )(got)


def output_kernel(value_ref, factor_ref, out_ref):
    high, low = split(factor_ref[...].T)
    factor = jnp.concatenate([high, high, low, low], axis=1)
    step = pl.program_id(0)
    for k in range(8):
        turned = value_ref[pl.ds(2 * k + step, 128, stride=16), :].T
        high, low = split(jnp.concatenate([turned[:64], turned[64:]], axis=1))
        out = dot(factor, jnp.concatenate([high, low, high, low], axis=0))
        for part in range(2):
            out_ref[part, 0, pl.ds(k, 128, stride=8), :] = out[:, part * LANES : (part + 1) * LANES]


def output_modes(values, factor):
    return pl.pallas_call(
        output_kernel,
        grid=(2,),
        in_specs=[
            pl.BlockSpec((2048, LANES), lambda i: (0, 0)),
            pl.BlockSpec((64, 128), lambda i: (0, 0)),
        ],
        out_specs=pl.BlockSpec((2, 1, 1024, LANES), lambda i: (0, i, 0, 0)),
        out_shape=jax.ShapeDtypeStruct((2, 2, 1024, LANES), jnp.float32),
        compiler_params=pltpu.CompilerParams(vmem_limit_bytes=VMEM_SMALL),
        name="output_modes",
    )(values, factor)


def swap(chunks, axes):
    return lax.all_to_all(chunks, axes, split_axis=0, concat_axis=0, tiled=True)


def per_device(
    spectrum, core_tensor, input_factor, output_factor, first_factor, second_factor, third_factor
):
    everyone = ("mx", "my", "col")
    count = lax.axis_size("my")
    seconds = [second_factor]
    for k in range(1, 4):
        pairs = [(b, b ^ k) for b in range(count)]
        seconds.append(lax.ppermute(second_factor, "my", pairs))
    core = jnp.transpose(core_tensor, (0, 1, 3, 4, 5, 2)).reshape(2, 8, 256, 64)
    spec = spectrum.reshape(2, 2, 1024, LANES)
    chunks, halves = spectrum_chunks(spec, core, input_factor.T, first_factor)
    chunks = core_chunks(chunks, halves, seconds, third_factor)
    got = swap(chunks.reshape(128, 1, CHUNK * LANES), everyone)
    values = mode_products(got.reshape(128 * CHUNK, LANES))
    values = swap(values.reshape(128, 16, LANES), everyone)
    out = output_modes(values.reshape(2048, LANES), output_factor.T)
    return out.reshape(spectrum.shape)


def solution(mesh):
    placed = (
        P(None, "col", None, "mx", "my"),
        P(None, "col", None, ("mx", "my"), None, None),
        P(),
        P(),
        P("mx", None),
        P("my", None),
        P(),
    )
    return jax.shard_map(
        per_device,
        mesh=mesh,
        in_specs=placed,
        out_specs=P(None, "col", None, "mx", "my"),
        check_vma=False,
    )
```

```python
import jax
import jax.numpy as jnp
from jax import lax
from jax.experimental import pallas as pl
from jax.experimental.pallas import tpu as pltpu
from jax.sharding import PartitionSpec as P


LANES = 128
SHARE = 65
WIDE = 72
VMEM_SMALL = 16 * 2**20
VMEM_ALONE = 56 * 2**20
VMEM_LARGE = 32 * 2**20


def dot(a, b):
    return jnp.dot(a, b, preferred_element_type=jnp.float32)


def split(x):
    high = x.astype(jnp.bfloat16)
    return high, (x - high.astype(jnp.float32)).astype(jnp.bfloat16)


def split3(x):
    high = x.astype(jnp.bfloat16)
    return (high, *split(x - high.astype(jnp.float32)))


def iota(shape, dim):
    return lax.broadcasted_iota(jnp.int32, shape, dim)


def pick(chosen, table):
    one = chosen.astype(jnp.bfloat16)
    high, mid, low = split3(table)
    return (dot(one, high) + dot(one, mid)) + dot(one, low)


def pick_lanes(table, chosen):
    one = chosen.astype(jnp.bfloat16)
    high, mid, low = split3(table)
    return (dot(high, one) + dot(mid, one)) + dot(low, one)


def spectrum_kernel(spec_hbm, in_hbm, first_hbm, out_ref, spec_ref, in_ref, first_ref, sems):
    def copy(source, target, n):
        made = pltpu.make_async_copy(source, target, sems.at[n])
        made.start()
        return made

    small = [copy(first_hbm, first_ref, 0), copy(in_hbm, in_ref, 1)]
    parts = [copy(spec_hbm.at[:, b], spec_ref.at[:, b], 2 + b) for b in range(2)]

    for made in small:
        made.wait()
    of_s = iota((16, 128), 1) & 15 == iota((16, 128), 0)
    mine = pick_lanes(first_ref[...], of_s)
    mine = jnp.where(iota((8, 128), 1) >> 4 == iota((8, 128), 0), mine, 0.0)
    mine = jnp.sum(mine, axis=0, keepdims=True)
    out_ref[pl.ds(64, 32, stride=SHARE), :] = jnp.broadcast_to(mine, (32, LANES))

    high, low = split(in_ref[...])
    rows = jnp.concatenate(
        [jnp.concatenate([high, high], axis=1), jnp.concatenate([low, low], axis=1)], axis=0
    )
    for made in parts:
        made.wait()
    for b in range(2):
        for k in range(8):
            both = jnp.concatenate(
                [spec_ref[part, b, pl.ds(k, 128, stride=8), :] for part in range(2)], axis=1
            )
            out = dot(rows, jnp.concatenate(split(both), axis=0))
            out = out[:64] + out[64:]
            turned = jnp.concatenate([out[:, :LANES], out[:, LANES:]], axis=0).T
            for r in range(4):
                row = 8 * k + 2 * r + b
                out_ref[pl.ds(row, 32, stride=SHARE), :] = turned[r * 32 : (r + 1) * 32]


def spectrum_chunks(spec, factor, first):
    return pl.pallas_call(
        spectrum_kernel,
        in_specs=[pl.BlockSpec(memory_space=pl.ANY)] * 3,
        out_shape=jax.ShapeDtypeStruct((32 * SHARE, LANES), jnp.float32),
        scratch_shapes=[
            pltpu.VMEM(spec.shape, jnp.float32),
            pltpu.VMEM(factor.shape, jnp.float32),
            pltpu.VMEM(first.shape, jnp.float32),
            pltpu.SemaphoreType.DMA((4,)),
        ],
        compiler_params=pltpu.CompilerParams(vmem_limit_bytes=VMEM_ALONE),
        name="spectrum_chunks",
    )(spec, factor, first)


def half_kernel(core_ref, half_ref):
    for pair in range(4):
        both = jnp.concatenate(
            [core_ref[part, 2 * pair + half] for half in range(2) for part in range(2)], axis=1
        )
        half_ref[pair, 0], half_ref[pair, 1] = split(both)


def core_halves(core):
    return pl.pallas_call(
        half_kernel,
        out_shape=pltpu.VMEM((4, 2, 256, 256), jnp.bfloat16),
        compiler_params=pltpu.CompilerParams(vmem_limit_bytes=VMEM_SMALL),
        name="core_halves",
    )(core)


def core_kernel(half_ref, s0_ref, s1_ref, s2_ref, s3_ref, third_ref, out_ref):
    own = lax.axis_index("my")
    seconds = jnp.concatenate([ref[...] for ref in (s0_ref, s1_ref, s2_ref, s3_ref)], axis=0)

    def place(width):
        row, col = iota((512, width), 0), iota((512, width), 1)
        c, b, a, r = row & 7, (row >> 3) & 3, (row >> 5) & 3, row >> 7
        return col, (b ^ own) * 8 + 2 * r + (a >> 1), (a & 1) * 8 + c

    of_t = iota((16, 256), 1) >> 4 == iota((16, 256), 0)
    of_u = iota((16, 256), 1) & 15 == iota((16, 256), 0)
    second, third = pick_lanes(seconds, of_t), pick_lanes(third_ref[...], of_u)
    col, ky, _ = place(32)
    by_y = pick(col == ky, second)
    col, _, kz = place(16)
    mat_high, mat_low = split(by_y * pick(col == kz, third))
    for pair in range(4):
        high, low = half_ref[pair, 0], half_ref[pair, 1]
        out = dot(mat_high, high) + dot(mat_high, low) + dot(mat_low, high)
        for half in range(2):
            for r in range(4):
                row = (2 * pair + half) * 4 + r
                out_ref[pl.ds(row, 128, stride=32), :] = out[
                    r * 128 : (r + 1) * 128, half * LANES : (half + 1) * LANES
                ]


def core_chunks(halves, seconds, third):
    return pl.pallas_call(
        core_kernel,
        out_shape=pltpu.VMEM((128 * 32, LANES), jnp.float32),
        compiler_params=pltpu.CompilerParams(vmem_limit_bytes=VMEM_SMALL),
        name="core_chunks",
    )(halves, *seconds, third)


def mode_kernel(core, spec, out_ref, w_ref):
    row, col = iota((256, 128), 0), iota((256, 128), 1)
    first = jnp.concatenate([spec[pl.ds(a * 8 * SHARE + 64, 1), :] for a in range(4)] * 2, axis=0)
    first = pick((iota((256, 8), 0) >> 5) & 3 == iota((256, 8), 1), first)
    first = jnp.where(col >> 4 == (row >> 2) & 7, first, 0.0)
    first = pick_lanes(first, iota((128, 128), 0) & 15 == iota((128, 128), 1) >> 3)
    same = ((row >> 7) == ((col >> 2) & 1)) & ((row & 3) == (col & 3))
    high, low = split(jnp.where(same, first, 0.0))
    expand = jnp.concatenate(
        [jnp.concatenate([high, high], axis=1), jnp.concatenate([low, low], axis=1)], axis=0
    )

    for src in range(8):
        for two in range(2):
            blocks = [
                jnp.concatenate(
                    [
                        core[pl.ds((s * 8 + src) * 32 + 8 * pair, 8), :]
                        for s in range(16)
                    ],
                    axis=0,
                )
                for pair in (2 * two, 2 * two + 1)
            ]
            out = dot(expand, jnp.concatenate(split(jnp.concatenate(blocks, axis=1)), axis=0))
            out = out[:256] + out[256:]
            for pair in range(2):
                for half in range(2):
                    p = src * 8 + (2 * two + pair) * 2 + half
                    w_ref[pl.ds(p, 128, stride=WIDE), :] = out[
                        half * 128 : (half + 1) * 128, pair * LANES : (pair + 1) * LANES
                    ]

    left = iota((16, LANES), 1) < 64

    out_ref[pl.ds(64, 32, stride=SHARE), :] = jnp.zeros((32, LANES), jnp.float32)
    for a in range(4):
        for kr in range(32):
            start = a * 8 * SHARE + 2 * kr
            x = jnp.concatenate(
                [spec[pl.ds(start + b, 8, stride=SHARE), :] for b in range(2)], axis=0
            )
            swapped = pltpu.roll(x, 64, 1)
            real, imag = jnp.where(left, x, swapped), jnp.where(left, swapped, x)
            rows = jnp.concatenate([*split(real), *split(imag)], axis=0)
            w = w_ref[pl.ds((a * 32 + kr) * WIDE, 64), :]
            out = dot(rows, jnp.concatenate(split(w), axis=0))
            by_real, by_imag = out[:16] + out[16:32], out[32:48] + out[48:]
            swapped = pltpu.roll(by_imag, 64, 1)
            value = by_real + jnp.where(left, -swapped, swapped)
            for b in range(2):
                out_ref[pl.ds(start + b, 8, stride=SHARE), :] = value[b * 8 : (b + 1) * 8]


def mode_products(core, spec):
    return pl.pallas_call(
        mode_kernel,
        out_shape=pltpu.VMEM((32 * SHARE, LANES), jnp.float32),
        scratch_shapes=[pltpu.VMEM((128 * WIDE, LANES), jnp.float32)],
        compiler_params=pltpu.CompilerParams(vmem_limit_bytes=VMEM_LARGE),
        name="mode_products",
    )(core, spec)


def output_kernel(value_ref, factor_ref, out_ref):
    high, low = split(factor_ref[...].T)
    factor = jnp.concatenate([high, high, low, low], axis=1)
    step = pl.program_id(0)
    for k in range(8):
        rows = [value_ref[pl.ds(8 * k + 2 * r + step, 32, stride=SHARE), :] for r in range(4)]
        turned = jnp.concatenate(rows, axis=0).T
        high, low = split(jnp.concatenate([turned[:64], turned[64:]], axis=1))
        out = dot(factor, jnp.concatenate([high, low, high, low], axis=0))
        for part in range(2):
            out_ref[part, 0, pl.ds(k, 128, stride=8), :] = out[:, part * LANES : (part + 1) * LANES]


def output_modes(values, factor):
    return pl.pallas_call(
        output_kernel,
        grid=(2,),
        in_specs=[
            pl.BlockSpec((32 * SHARE, LANES), lambda i: (0, 0)),
            pl.BlockSpec((64, 128), lambda i: (0, 0)),
        ],
        out_specs=pl.BlockSpec((2, 1, 1024, LANES), lambda i: (0, i, 0, 0)),
        out_shape=jax.ShapeDtypeStruct((2, 2, 1024, LANES), jnp.float32),
        compiler_params=pltpu.CompilerParams(vmem_limit_bytes=VMEM_SMALL),
        name="output_modes",
    )(values, factor)


def swap(chunks, axes):
    return lax.all_to_all(chunks, axes, split_axis=0, concat_axis=0, tiled=True)


def per_device(
    spectrum, core_tensor, input_factor, output_factor, first_factor, second_factor, third_factor
):
    count = lax.axis_size("my")
    spec = spectrum.reshape(2, 2, 1024, LANES)
    spec = spectrum_chunks(spec, input_factor.T, first_factor)
    spec = swap(spec.reshape(32, 1, SHARE * LANES), ("mx", "col"))
    seconds = [second_factor]
    for k in range(1, 4):
        pairs = [(b, b ^ k) for b in range(count)]
        seconds.append(lax.ppermute(second_factor, "my", pairs))
    core = jnp.transpose(core_tensor, (0, 1, 3, 4, 5, 2)).reshape(2, 8, 256, 64)
    halves = core_halves(core)
    core = core_chunks(halves, seconds, third_factor)
    core = swap(core.reshape(128, 32, LANES), ("mx", "my", "col"))
    values = mode_products(core.reshape(128 * 32, LANES), spec.reshape(32 * SHARE, LANES))
    values = swap(values.reshape(32, 1, SHARE * LANES), ("mx", "col"))
    out = output_modes(values.reshape(32 * SHARE, LANES), output_factor.T)
    return out.reshape(spectrum.shape)


def solution(mesh):
    placed = (
        P(None, "col", None, "mx", "my"),
        P(None, "col", None, ("mx", "my"), None, None),
        P(),
        P(),
        P("mx", None),
        P("my", None),
        P(),
    )
    return jax.shard_map(
        per_device,
        mesh=mesh,
        in_specs=placed,
        out_specs=P(None, "col", None, "mx", "my"),
        check_vma=False,
    )
```

```python
import jax
import jax.numpy as jnp
from jax import lax
from jax.experimental import pallas as pl
from jax.experimental.pallas import tpu as pltpu
from jax.sharding import PartitionSpec as P


LANES = 128
CHUNK = 49
WIDE = 72
VMEM_SMALL = 16 * 2**20
VMEM_ALONE = 56 * 2**20
VMEM_LARGE = 32 * 2**20


def dot(a, b):
    return jnp.dot(a, b, preferred_element_type=jnp.float32)


def split(x):
    high = x.astype(jnp.bfloat16)
    return high, (x - high.astype(jnp.float32)).astype(jnp.bfloat16)


def split3(x):
    high = x.astype(jnp.bfloat16)
    return (high, *split(x - high.astype(jnp.float32)))


def iota(shape, dim):
    return lax.broadcasted_iota(jnp.int32, shape, dim)


def pick(chosen, table):
    one = chosen.astype(jnp.bfloat16)
    high, mid, low = split3(table)
    return (dot(one, high) + dot(one, mid)) + dot(one, low)


def pick_lanes(table, chosen):
    one = chosen.astype(jnp.bfloat16)
    high, mid, low = split3(table)
    return (dot(high, one) + dot(mid, one)) + dot(low, one)


def spectrum_kernel(
    spec_hbm, core_hbm, in_hbm, first_hbm, third_hbm, out_ref, half_ref, by_z_ref,
    spec_ref, core_ref, in_ref, first_ref, third_ref, sems,
):
    def copy(source, target, n):
        made = pltpu.make_async_copy(source, target, sems.at[n])
        made.start()
        return made

    small = [copy(first_hbm, first_ref, 0), copy(in_hbm, in_ref, 1), copy(third_hbm, third_ref, 2)]
    parts = [copy(spec_hbm.at[:, b], spec_ref.at[:, b], 3 + b) for b in range(2)]
    parts.append(copy(core_hbm, core_ref, 5))

    for made in small:
        made.wait()
    of_s = iota((16, 128), 1) & 15 == iota((16, 128), 0)
    mine = pick_lanes(first_ref[...], of_s)
    mine = jnp.where(iota((8, 128), 1) >> 4 == iota((8, 128), 0), mine, 0.0)
    mine = jnp.sum(mine, axis=0, keepdims=True)
    out_ref[pl.ds(48, 128, stride=CHUNK), :] = jnp.broadcast_to(mine, (128, LANES))

    high, low = split(in_ref[...])
    rows = jnp.concatenate(
        [jnp.concatenate([high, high], axis=1), jnp.concatenate([low, low], axis=1)], axis=0
    )
    of_u = iota((16, 256), 1) & 15 == iota((16, 256), 0)
    third = pick_lanes(third_ref[...], of_u)
    by_z_ref[...] = pick(iota((128, 16), 0) & 15 == iota((128, 16), 1), third)
    for b in range(2):
        parts[b].wait()
        for k in range(8):
            both = jnp.concatenate(
                [spec_ref[part, b, pl.ds(k, 128, stride=8), :] for part in range(2)], axis=1
            )
            out = dot(rows, jnp.concatenate(split(both), axis=0))
            out = out[:64] + out[64:]
            turned = jnp.concatenate([out[:, :LANES], out[:, LANES:]], axis=0).T
            out_ref[pl.ds(2 * k + b, 128, stride=CHUNK), :] = turned
    parts[2].wait()
    for pair in range(4):
        both = jnp.concatenate(
            [core_ref[part, 2 * pair + half] for half in range(2) for part in range(2)], axis=1
        )
        half_ref[pair, 0], half_ref[pair, 1] = split(both)


def spectrum_chunks(spec, core, factor, first, third):
    return pl.pallas_call(
        spectrum_kernel,
        in_specs=[pl.BlockSpec(memory_space=pl.ANY)] * 5,
        out_shape=(
            pltpu.VMEM((128 * CHUNK, LANES), jnp.float32),
            pltpu.VMEM((4, 2, 256, 256), jnp.bfloat16),
            pltpu.VMEM((128, 256), jnp.float32),
        ),
        scratch_shapes=[
            pltpu.VMEM(spec.shape, jnp.float32),
            pltpu.VMEM(core.shape, jnp.float32),
            pltpu.VMEM(factor.shape, jnp.float32),
            pltpu.VMEM(first.shape, jnp.float32),
            pltpu.VMEM(third.shape, jnp.float32),
            pltpu.SemaphoreType.DMA((6,)),
        ],
        compiler_params=pltpu.CompilerParams(vmem_limit_bytes=VMEM_ALONE),
        name="spectrum_chunks",
    )(spec, core, factor, first, third)


def core_kernel(_, half_ref, by_z_ref, s0_ref, s1_ref, s2_ref, s3_ref, out_ref):
    b = lax.axis_index("my")
    seconds = jnp.concatenate([ref[...] for ref in (s0_ref, s1_ref, s2_ref, s3_ref)], axis=0)
    of_t = iota((16, 256), 1) >> 4 == iota((16, 256), 0)
    second = pick_lanes(seconds, of_t)
    row = iota((512, 32), 0)
    by_y = pick(((row >> 7) ^ b) * 8 + ((row & 127) >> 4) == iota((512, 32), 1), second)
    by_z = jnp.concatenate([by_z_ref[...]] * 4, axis=0)
    mat_high, mat_low = split(by_y * by_z)
    for pair in range(4):
        high, low = half_ref[pair, 0], half_ref[pair, 1]
        out = dot(mat_high, high) + dot(mat_high, low) + dot(mat_low, high)
        for half in range(2):
            for r in range(4):
                row = 16 + (2 * pair + half) * 4 + r
                out_ref[pl.ds(row, 128, stride=CHUNK), :] = out[
                    r * 128 : (r + 1) * 128, half * LANES : (half + 1) * LANES
                ]


def core_chunks(chunks, halves, by_z, seconds):
    whole = pl.BlockSpec(memory_space=pltpu.VMEM)
    return pl.pallas_call(
        core_kernel,
        in_specs=[pl.BlockSpec(memory_space=pl.ANY)] + [whole] * 6,
        out_shape=pltpu.VMEM((128 * CHUNK, LANES), jnp.float32),
        input_output_aliases={0: 0},
        compiler_params=pltpu.CompilerParams(vmem_limit_bytes=VMEM_SMALL),
        name="core_chunks",
    )(chunks, halves, by_z, *seconds)


def mode_kernel(got, out_ref, w_ref):
    row, col = iota((128, 128), 0), iota((128, 128), 1)
    first = jnp.concatenate([got[pl.ds(a * 32 * CHUNK + 48, 1), :] for a in range(4)] * 2, axis=0)
    first = pick(iota((128, 8), 0) >> 5 == iota((128, 8), 1), first)
    first = jnp.where(col >> 4 == row & 7, first, 0.0)
    first = pick_lanes(first, row & 15 == col & 15)
    high, low = split(jnp.where((row >> 3) & 3 == (col >> 4) & 3, first, 0.0))
    expand = jnp.concatenate([high, low], axis=1)

    for pair in range(32):
        src, two = pair // 4, pair % 4
        block = jnp.concatenate(
            [
                jnp.concatenate(
                    [
                        got[pl.ds(src * CHUNK + 16 + (2 * two + half) * 4 + r, 16, stride=8 * CHUNK), :]
                        for r in range(4)
                    ],
                    axis=0,
                )
                for half in range(2)
            ],
            axis=1,
        )
        high, low = split(block)
        out = dot(expand, jnp.concatenate([high, low, high, low], axis=0))
        for half in range(2):
            w_ref[pl.ds(src * 8 + 2 * two + half, 128, stride=WIDE), :] = out[
                :, half * LANES : (half + 1) * LANES
            ]

    left = iota((16, LANES), 1) < 64

    for g in range(16):
        for k in range(8):
            x = jnp.concatenate(
                [got[pl.ds(g * 8 * CHUNK + 2 * k + b, 8, stride=CHUNK), :] for b in range(2)],
                axis=0,
            )
            swapped = pltpu.roll(x, 64, 1)
            real, imag = jnp.where(left, x, swapped), jnp.where(left, swapped, x)
            rows = jnp.concatenate([*split(real), *split(imag)], axis=0)
            w = w_ref[pl.ds((g * 8 + k) * WIDE, 64), :]
            out = dot(rows, jnp.concatenate(split(w), axis=0))
            by_real, by_imag = out[:16] + out[16:32], out[32:48] + out[48:]
            swapped = pltpu.roll(by_imag, 64, 1)
            value = by_real + jnp.where(left, -swapped, swapped)
            for b in range(2):
                out_ref[pl.ds(g * 128 + 2 * k + b, 8, stride=16), :] = value[b * 8 : (b + 1) * 8]


def mode_products(got):
    return pl.pallas_call(
        mode_kernel,
        out_shape=jax.ShapeDtypeStruct((128 * 16, LANES), jnp.float32),
        scratch_shapes=[pltpu.VMEM((128 * WIDE, LANES), jnp.float32)],
        compiler_params=pltpu.CompilerParams(vmem_limit_bytes=VMEM_LARGE),
        name="mode_products",
    )(got)


def output_kernel(value_ref, factor_ref, out_ref):
    high, low = split(factor_ref[...].T)
    factor = jnp.concatenate([high, high, low, low], axis=1)
    step = pl.program_id(0)
    for k in range(8):
        turned = value_ref[pl.ds(2 * k + step, 128, stride=16), :].T
        high, low = split(jnp.concatenate([turned[:64], turned[64:]], axis=1))
        out = dot(factor, jnp.concatenate([high, low, high, low], axis=0))
        for part in range(2):
            out_ref[part, 0, pl.ds(k, 128, stride=8), :] = out[:, part * LANES : (part + 1) * LANES]


def output_modes(values, factor):
    return pl.pallas_call(
        output_kernel,
        grid=(2,),
        in_specs=[
            pl.BlockSpec((2048, LANES), lambda i: (0, 0)),
            pl.BlockSpec((64, 128), lambda i: (0, 0)),
        ],
        out_specs=pl.BlockSpec((2, 1, 1024, LANES), lambda i: (0, i, 0, 0)),
        out_shape=jax.ShapeDtypeStruct((2, 2, 1024, LANES), jnp.float32),
        compiler_params=pltpu.CompilerParams(vmem_limit_bytes=VMEM_SMALL),
        name="output_modes",
    )(values, factor)


def swap(chunks, axes):
    return lax.all_to_all(chunks, axes, split_axis=0, concat_axis=0, tiled=True)


def per_device(
    spectrum, core_tensor, input_factor, output_factor, first_factor, second_factor, third_factor
):
    everyone = ("mx", "my", "col")
    count = lax.axis_size("my")
    seconds = [second_factor]
    for k in range(1, 4):
        pairs = [(b, b ^ k) for b in range(count)]
        seconds.append(lax.ppermute(second_factor, "my", pairs))
    core = jnp.transpose(core_tensor, (0, 1, 3, 4, 5, 2)).reshape(2, 8, 256, 64)
    spec = spectrum.reshape(2, 2, 1024, LANES)
    chunks, halves, by_z = spectrum_chunks(spec, core, input_factor.T, first_factor, third_factor)
    chunks = core_chunks(chunks, halves, by_z, seconds)
    got = swap(chunks.reshape(128, 1, CHUNK * LANES), everyone)
    values = mode_products(got.reshape(128 * CHUNK, LANES))
    values = swap(values.reshape(128, 16, LANES), everyone)
    out = output_modes(values.reshape(2048, LANES), output_factor.T)
    return out.reshape(spectrum.shape)


def solution(mesh):
    placed = (
        P(None, "col", None, "mx", "my"),
        P(None, "col", None, ("mx", "my"), None, None),
        P(),
        P(),
        P("mx", None),
        P("my", None),
        P(),
    )
    return jax.shard_map(
        per_device,
        mesh=mesh,
        in_specs=placed,
        out_specs=P(None, "col", None, "mx", "my"),
        check_vma=False,
    )
```

```python
import jax
import jax.numpy as jnp
from jax import lax
from jax.experimental import pallas as pl
from jax.experimental.pallas import tpu as pltpu
from jax.sharding import PartitionSpec as P


LANES = 128
CHUNK = 49
WIDE = 65
VMEM_SMALL = 16 * 2**20
VMEM_ALONE = 56 * 2**20
VMEM_LARGE = 32 * 2**20


def dot(a, b):
    return jnp.dot(a, b, preferred_element_type=jnp.float32)


def split(x):
    high = x.astype(jnp.bfloat16)
    return high, (x - high.astype(jnp.float32)).astype(jnp.bfloat16)


def split3(x):
    high = x.astype(jnp.bfloat16)
    return (high, *split(x - high.astype(jnp.float32)))


def iota(shape, dim):
    return lax.broadcasted_iota(jnp.int32, shape, dim)


def pick(chosen, table):
    one = chosen.astype(jnp.bfloat16)
    high, mid, low = split3(table)
    return (dot(one, high) + dot(one, mid)) + dot(one, low)


def pick_lanes(table, chosen):
    one = chosen.astype(jnp.bfloat16)
    high, mid, low = split3(table)
    return (dot(high, one) + dot(mid, one)) + dot(low, one)


def spectrum_kernel(
    spec_hbm, core_hbm, in_hbm, first_hbm, third_hbm, out_ref, half_ref, by_z_ref,
    spec_ref, core_ref, in_ref, first_ref, third_ref, sems,
):
    def copy(source, target, n):
        made = pltpu.make_async_copy(source, target, sems.at[n])
        made.start()
        return made

    small = [copy(first_hbm, first_ref, 0), copy(in_hbm, in_ref, 1), copy(third_hbm, third_ref, 2)]
    parts = [copy(spec_hbm.at[:, b], spec_ref.at[:, b], 3 + b) for b in range(2)]
    parts.append(copy(core_hbm, core_ref, 5))

    for made in small:
        made.wait()
    of_s = iota((16, 128), 1) & 15 == iota((16, 128), 0)
    mine = pick_lanes(first_ref[...], of_s)
    mine = jnp.where(iota((8, 128), 1) >> 4 == iota((8, 128), 0), mine, 0.0)
    mine = jnp.sum(mine, axis=0, keepdims=True)
    out_ref[pl.ds(48, 128, stride=CHUNK), :] = jnp.broadcast_to(mine, (128, LANES))

    high, low = split(in_ref[...])
    rows = jnp.concatenate(
        [jnp.concatenate([high, high], axis=1), jnp.concatenate([low, low], axis=1)], axis=0
    )
    of_u = iota((16, 256), 1) & 15 == iota((16, 256), 0)
    third = pick_lanes(third_ref[...], of_u)
    by_z_ref[...] = pick(iota((128, 16), 0) & 15 == iota((128, 16), 1), third)
    for b in range(2):
        parts[b].wait()
        for k in range(8):
            both = jnp.concatenate(
                [spec_ref[part, b, pl.ds(k, 128, stride=8), :] for part in range(2)], axis=1
            )
            out = dot(rows, jnp.concatenate(split(both), axis=0))
            out = out[:64] + out[64:]
            turned = jnp.concatenate([out[:, :LANES], out[:, LANES:]], axis=0).T
            out_ref[pl.ds(2 * k + b, 128, stride=CHUNK), :] = turned
    parts[2].wait()
    for pair in range(4):
        both = jnp.concatenate(
            [core_ref[part, 2 * pair + half] for half in range(2) for part in range(2)], axis=1
        )
        half_ref[pair, 0], half_ref[pair, 1] = split(both)


def spectrum_chunks(spec, core, factor, first, third):
    return pl.pallas_call(
        spectrum_kernel,
        in_specs=[pl.BlockSpec(memory_space=pl.ANY)] * 5,
        out_shape=(
            pltpu.VMEM((128 * CHUNK, LANES), jnp.float32),
            pltpu.VMEM((4, 2, 256, 256), jnp.bfloat16),
            pltpu.VMEM((128, 256), jnp.float32),
        ),
        scratch_shapes=[
            pltpu.VMEM(spec.shape, jnp.float32),
            pltpu.VMEM(core.shape, jnp.float32),
            pltpu.VMEM(factor.shape, jnp.float32),
            pltpu.VMEM(first.shape, jnp.float32),
            pltpu.VMEM(third.shape, jnp.float32),
            pltpu.SemaphoreType.DMA((6,)),
        ],
        compiler_params=pltpu.CompilerParams(vmem_limit_bytes=VMEM_ALONE),
        name="spectrum_chunks",
    )(spec, core, factor, first, third)


def core_kernel(_, half_ref, by_z_ref, s0_ref, s1_ref, s2_ref, s3_ref, out_ref):
    b = lax.axis_index("my")
    seconds = jnp.concatenate([ref[...] for ref in (s0_ref, s1_ref, s2_ref, s3_ref)], axis=0)
    of_t = iota((16, 256), 1) >> 4 == iota((16, 256), 0)
    second = pick_lanes(seconds, of_t)
    row = iota((512, 32), 0)
    by_y = pick(((row >> 7) ^ b) * 8 + ((row & 127) >> 4) == iota((512, 32), 1), second)
    by_z = jnp.concatenate([by_z_ref[...]] * 4, axis=0)
    mat_high, mat_low = split(by_y * by_z)
    for pair in range(4):
        high, low = half_ref[pair, 0], half_ref[pair, 1]
        out = dot(mat_high, high) + dot(mat_high, low) + dot(mat_low, high)
        for half in range(2):
            for r in range(4):
                row = 16 + (2 * pair + half) * 4 + r
                out_ref[pl.ds(row, 128, stride=CHUNK), :] = out[
                    r * 128 : (r + 1) * 128, half * LANES : (half + 1) * LANES
                ]


def core_chunks(chunks, halves, by_z, seconds):
    whole = pl.BlockSpec(memory_space=pltpu.VMEM)
    return pl.pallas_call(
        core_kernel,
        in_specs=[pl.BlockSpec(memory_space=pl.ANY)] + [whole] * 6,
        out_shape=pltpu.VMEM((128 * CHUNK, LANES), jnp.float32),
        input_output_aliases={0: 0},
        compiler_params=pltpu.CompilerParams(vmem_limit_bytes=VMEM_SMALL),
        name="core_chunks",
    )(chunks, halves, by_z, *seconds)


def mode_kernel(got, out_ref, w_ref):
    row, col = iota((128, 128), 0), iota((128, 128), 1)
    first = jnp.concatenate([got[pl.ds(a * 32 * CHUNK + 48, 1), :] for a in range(4)] * 2, axis=0)
    first = pick(iota((128, 8), 0) >> 5 == iota((128, 8), 1), first)
    first = jnp.where(col >> 4 == row & 7, first, 0.0)
    first = pick_lanes(first, row & 15 == col & 15)
    high, low = split(jnp.where((row >> 3) & 3 == (col >> 4) & 3, first, 0.0))
    expand = jnp.concatenate([high, low], axis=1)

    for pair in range(32):
        src, two = pair // 4, pair % 4
        block = jnp.concatenate(
            [
                jnp.concatenate(
                    [
                        got[pl.ds(src * CHUNK + 16 + (2 * two + half) * 4 + r, 16, stride=8 * CHUNK), :]
                        for r in range(4)
                    ],
                    axis=0,
                )
                for half in range(2)
            ],
            axis=1,
        )
        high, low = split(block)
        out = dot(expand, jnp.concatenate([high, low, high, low], axis=0))
        for half in range(2):
            w_ref[pl.ds(src * 8 + 2 * two + half, 128, stride=WIDE), :] = out[
                :, half * LANES : (half + 1) * LANES
            ]

    left = iota((16, LANES), 1) < 64
    sign = jnp.where(left, -1.0, 1.0)

    for g in range(16):
        for k in range(8):
            x = jnp.concatenate(
                [got[pl.ds(g * 8 * CHUNK + 2 * k + b, 8, stride=CHUNK), :] for b in range(2)],
                axis=0,
            )
            swapped = pltpu.roll(x, 64, 1)
            real, imag = jnp.where(left, x, swapped), jnp.where(left, swapped, x)
            rows = jnp.concatenate([*split(real), *split(imag)], axis=0)
            w = w_ref[pl.ds((g * 8 + k) * WIDE, 64), :]
            out = dot(rows, jnp.concatenate(split(w), axis=0))
            by_real, by_imag = out[:16] + out[16:32], out[32:48] + out[48:]
            swapped = pltpu.roll(by_imag, 64, 1)
            value = by_real + sign * swapped
            for b in range(2):
                out_ref[pl.ds(g * 128 + 2 * k + b, 8, stride=16), :] = value[b * 8 : (b + 1) * 8]


def mode_products(got):
    return pl.pallas_call(
        mode_kernel,
        out_shape=jax.ShapeDtypeStruct((128 * 16, LANES), jnp.float32),
        scratch_shapes=[pltpu.VMEM((128 * WIDE, LANES), jnp.float32)],
        compiler_params=pltpu.CompilerParams(vmem_limit_bytes=VMEM_LARGE),
        name="mode_products",
    )(got)


def output_kernel(value_ref, factor_ref, out_hbm, out_ref, sems):
    high, low = split(factor_ref[...].T)
    factor = jnp.concatenate([high, high, low, low], axis=1)
    copies = [
        pltpu.make_async_copy(out_ref.at[:, b], out_hbm.at[:, b], sems.at[b]) for b in range(2)
    ]
    for b in range(2):
        for k in range(8):
            turned = value_ref[pl.ds(2 * k + b, 128, stride=16), :].T
            high, low = split(jnp.concatenate([turned[:64], turned[64:]], axis=1))
            out = dot(factor, jnp.concatenate([high, low, high, low], axis=0))
            for part in range(2):
                out_ref[part, b, pl.ds(k, 128, stride=8), :] = out[
                    :, part * LANES : (part + 1) * LANES
                ]
        copies[b].start()
    for copy in copies:
        copy.wait()


def output_modes(values, factor):
    whole = (2, 2, 1024, LANES)
    return pl.pallas_call(
        output_kernel,
        out_specs=pl.BlockSpec(memory_space=pl.ANY),
        out_shape=jax.ShapeDtypeStruct(whole, jnp.float32),
        scratch_shapes=[pltpu.VMEM(whole, jnp.float32), pltpu.SemaphoreType.DMA((2,))],
        compiler_params=pltpu.CompilerParams(vmem_limit_bytes=VMEM_SMALL),
        name="output_modes",
    )(values, factor)


def swap(chunks, axes):
    return lax.all_to_all(chunks, axes, split_axis=0, concat_axis=0, tiled=True)


def per_device(
    spectrum, core_tensor, input_factor, output_factor, first_factor, second_factor, third_factor
):
    everyone = ("mx", "my", "col")
    count = lax.axis_size("my")
    seconds = [second_factor]
    for k in range(1, 4):
        pairs = [(b, b ^ k) for b in range(count)]
        seconds.append(lax.ppermute(second_factor, "my", pairs))
    core = jnp.transpose(core_tensor, (0, 1, 3, 4, 5, 2)).reshape(2, 8, 256, 64)
    spec = spectrum.reshape(2, 2, 1024, LANES)
    chunks, halves, by_z = spectrum_chunks(spec, core, input_factor.T, first_factor, third_factor)
    chunks = core_chunks(chunks, halves, by_z, seconds)
    got = swap(chunks.reshape(128, 1, CHUNK * LANES), everyone)
    values = mode_products(got.reshape(128 * CHUNK, LANES))
    values = swap(values.reshape(128, 16, LANES), everyone)
    out = output_modes(values.reshape(2048, LANES), output_factor.T)
    return out.reshape(spectrum.shape)


def solution(mesh):
    placed = (
        P(None, "col", None, "mx", "my"),
        P(None, "col", None, ("mx", "my"), None, None),
        P(),
        P(),
        P("mx", None),
        P("my", None),
        P(),
    )
    return jax.shard_map(
        per_device,
        mesh=mesh,
        in_specs=placed,
        out_specs=P(None, "col", None, "mx", "my"),
        check_vma=False,
    )
```

```python
import jax
import jax.numpy as jnp
from jax import lax
from jax.experimental import pallas as pl
from jax.experimental.pallas import tpu as pltpu
from jax.sharding import PartitionSpec as P


LANES = 128
CHUNK = 49
WIDE = 65
VMEM_SMALL = 16 * 2**20
VMEM_ALONE = 56 * 2**20
VMEM_LARGE = 32 * 2**20


def dot(a, b):
    return jnp.dot(a, b, preferred_element_type=jnp.float32)


def split(x):
    high = x.astype(jnp.bfloat16)
    return high, (x - high.astype(jnp.float32)).astype(jnp.bfloat16)


def split3(x):
    high = x.astype(jnp.bfloat16)
    return (high, *split(x - high.astype(jnp.float32)))


def iota(shape, dim):
    return lax.broadcasted_iota(jnp.int32, shape, dim)


def pick(rows, chosen, table):
    shape = (rows, 3 * table.shape[0])
    one = chosen(iota(shape, 0), iota(shape, 1) & (table.shape[0] - 1)).astype(jnp.bfloat16)
    return dot(one, jnp.concatenate(split3(table), axis=0))


def pick_lanes(table, lanes, chosen):
    shape = (3 * table.shape[1], lanes)
    one = chosen(iota(shape, 0) & (table.shape[1] - 1), iota(shape, 1)).astype(jnp.bfloat16)
    return dot(jnp.concatenate(split3(table), axis=1), one)


def spectrum_kernel(
    spec_hbm, core_hbm, in_hbm, first_hbm, third_hbm, out_ref, half_ref, by_z_ref,
    spec_ref, core_ref, in_ref, first_ref, third_ref, sems,
):
    def copy(source, target, n):
        made = pltpu.make_async_copy(source, target, sems.at[n])
        made.start()
        return made

    small = [copy(first_hbm, first_ref, 0), copy(in_hbm, in_ref, 1), copy(third_hbm, third_ref, 2)]
    parts = [copy(spec_hbm.at[:, b], spec_ref.at[:, b], 3 + b) for b in range(2)]
    parts.append(copy(core_hbm, core_ref, 5))

    for made in small:
        made.wait()
    mine = pick_lanes(first_ref[...], 128, lambda row, col: col & 15 == row)
    mine = jnp.where(iota((8, 128), 1) >> 4 == iota((8, 128), 0), mine, 0.0)
    mine = jnp.sum(mine, axis=0, keepdims=True)
    out_ref[pl.ds(48, 128, stride=CHUNK), :] = jnp.broadcast_to(mine, (128, LANES))

    high, low = split(in_ref[...])
    rows = jnp.concatenate(
        [jnp.concatenate([high, high], axis=1), jnp.concatenate([low, low], axis=1)], axis=0
    )
    third = pick_lanes(third_ref[...], 256, lambda row, col: col & 15 == row)
    by_z_ref[...] = pick(128, lambda row, col: row & 15 == col, third)
    for b in range(2):
        parts[b].wait()
        for k in range(8):
            both = jnp.concatenate(
                [spec_ref[part, b, pl.ds(k, 128, stride=8), :] for part in range(2)], axis=1
            )
            out = dot(rows, jnp.concatenate(split(both), axis=0))
            out = out[:64] + out[64:]
            turned = jnp.concatenate([out[:, :LANES], out[:, LANES:]], axis=0).T
            out_ref[pl.ds(2 * k + b, 128, stride=CHUNK), :] = turned
    parts[2].wait()
    for pair in range(4):
        both = jnp.concatenate(
            [core_ref[part, 2 * pair + half] for half in range(2) for part in range(2)], axis=1
        )
        half_ref[pair, 0], half_ref[pair, 1] = split(both)


def spectrum_chunks(spec, core, factor, first, third):
    return pl.pallas_call(
        spectrum_kernel,
        in_specs=[pl.BlockSpec(memory_space=pl.ANY)] * 5,
        out_shape=(
            pltpu.VMEM((128 * CHUNK, LANES), jnp.float32),
            pltpu.VMEM((4, 2, 256, 256), jnp.bfloat16),
            pltpu.VMEM((128, 256), jnp.float32),
        ),
        scratch_shapes=[
            pltpu.VMEM(spec.shape, jnp.float32),
            pltpu.VMEM(core.shape, jnp.float32),
            pltpu.VMEM(factor.shape, jnp.float32),
            pltpu.VMEM(first.shape, jnp.float32),
            pltpu.VMEM(third.shape, jnp.float32),
            pltpu.SemaphoreType.DMA((6,)),
        ],
        compiler_params=pltpu.CompilerParams(vmem_limit_bytes=VMEM_ALONE),
        name="spectrum_chunks",
    )(spec, core, factor, first, third)


def core_kernel(_, half_ref, by_z_ref, s0_ref, s1_ref, s2_ref, s3_ref, out_ref):
    b = lax.axis_index("my")
    seconds = jnp.concatenate([ref[...] for ref in (s0_ref, s1_ref, s2_ref, s3_ref)], axis=0)
    second = pick_lanes(seconds, 256, lambda row, col: col >> 4 == row)
    by_y = pick(
        512, lambda row, col: ((row >> 7) ^ b) * 8 + ((row & 127) >> 4) == col, second
    )
    by_z = jnp.concatenate([by_z_ref[...]] * 4, axis=0)
    mat_high, mat_low = split(by_y * by_z)
    for pair in range(4):
        high, low = half_ref[pair, 0], half_ref[pair, 1]
        out = dot(mat_high, high) + dot(mat_high, low) + dot(mat_low, high)
        for half in range(2):
            for r in range(4):
                row = 16 + (2 * pair + half) * 4 + r
                out_ref[pl.ds(row, 128, stride=CHUNK), :] = out[
                    r * 128 : (r + 1) * 128, half * LANES : (half + 1) * LANES
                ]


def core_chunks(chunks, halves, by_z, seconds):
    whole = pl.BlockSpec(memory_space=pltpu.VMEM)
    return pl.pallas_call(
        core_kernel,
        in_specs=[pl.BlockSpec(memory_space=pl.ANY)] + [whole] * 6,
        out_shape=pltpu.VMEM((128 * CHUNK, LANES), jnp.float32),
        input_output_aliases={0: 0},
        compiler_params=pltpu.CompilerParams(vmem_limit_bytes=VMEM_SMALL),
        name="core_chunks",
    )(chunks, halves, by_z, *seconds)


def mode_kernel(got, out_ref, w_ref):
    row, col = iota((128, 128), 0), iota((128, 128), 1)
    first = jnp.concatenate([got[pl.ds(a * 32 * CHUNK + 48, 1), :] for a in range(4)] * 2, axis=0)
    first = pick(128, lambda row, col: row >> 5 == col, first)
    first = jnp.where(col >> 4 == row & 7, first, 0.0)
    first = pick_lanes(first, 128, lambda row, col: row & 15 == col & 15)
    high, low = split(jnp.where((row >> 3) & 3 == (col >> 4) & 3, first, 0.0))
    expand = jnp.concatenate([high, low], axis=1)

    for pair in range(32):
        src, two = pair // 4, pair % 4
        block = jnp.concatenate(
            [
                jnp.concatenate(
                    [
                        got[pl.ds(src * CHUNK + 16 + (2 * two + half) * 4 + r, 16, stride=8 * CHUNK), :]
                        for r in range(4)
                    ],
                    axis=0,
                )
                for half in range(2)
            ],
            axis=1,
        )
        high, low = split(block)
        out = dot(expand, jnp.concatenate([high, low, high, low], axis=0))
        for half in range(2):
            w_ref[pl.ds(src * 8 + 2 * two + half, 128, stride=WIDE), :] = out[
                :, half * LANES : (half + 1) * LANES
            ]

    left = iota((16, LANES), 1) < 64
    sign = jnp.where(left, -1.0, 1.0)

    for g in range(16):
        for k in range(8):
            x = jnp.concatenate(
                [got[pl.ds(g * 8 * CHUNK + 2 * k + b, 8, stride=CHUNK), :] for b in range(2)],
                axis=0,
            )
            swapped = pltpu.roll(x, 64, 1)
            real, imag = jnp.where(left, x, swapped), jnp.where(left, swapped, x)
            rows = jnp.concatenate([*split(real), *split(imag)], axis=0)
            w = w_ref[pl.ds((g * 8 + k) * WIDE, 64), :]
            out = dot(rows, jnp.concatenate(split(w), axis=0))
            by_real, by_imag = out[:16] + out[16:32], out[32:48] + out[48:]
            swapped = pltpu.roll(by_imag, 64, 1)
            value = by_real + sign * swapped
            for b in range(2):
                out_ref[pl.ds(g * 128 + 2 * k + b, 8, stride=16), :] = value[b * 8 : (b + 1) * 8]


def mode_products(got):
    return pl.pallas_call(
        mode_kernel,
        out_shape=jax.ShapeDtypeStruct((128 * 16, LANES), jnp.float32),
        scratch_shapes=[pltpu.VMEM((128 * WIDE, LANES), jnp.float32)],
        compiler_params=pltpu.CompilerParams(vmem_limit_bytes=VMEM_LARGE),
        name="mode_products",
    )(got)


def output_kernel(value_ref, factor_ref, out_hbm, out_ref, sems):
    high, low = split(factor_ref[...].T)
    factor = jnp.concatenate([high, high, low, low], axis=1)
    copies = [
        pltpu.make_async_copy(out_ref.at[:, b], out_hbm.at[:, b], sems.at[b]) for b in range(2)
    ]
    for b in range(2):
        for k in range(8):
            turned = value_ref[pl.ds(2 * k + b, 128, stride=16), :].T
            high, low = split(jnp.concatenate([turned[:64], turned[64:]], axis=1))
            out = dot(factor, jnp.concatenate([high, low, high, low], axis=0))
            for part in range(2):
                out_ref[part, b, pl.ds(k, 128, stride=8), :] = out[
                    :, part * LANES : (part + 1) * LANES
                ]
        copies[b].start()
    for copy in copies:
        copy.wait()


def output_modes(values, factor):
    whole = (2, 2, 1024, LANES)
    return pl.pallas_call(
        output_kernel,
        out_specs=pl.BlockSpec(memory_space=pl.ANY),
        out_shape=jax.ShapeDtypeStruct(whole, jnp.float32),
        scratch_shapes=[pltpu.VMEM(whole, jnp.float32), pltpu.SemaphoreType.DMA((2,))],
        compiler_params=pltpu.CompilerParams(vmem_limit_bytes=VMEM_SMALL),
        name="output_modes",
    )(values, factor)


def swap(chunks, axes):
    return lax.all_to_all(chunks, axes, split_axis=0, concat_axis=0, tiled=True)


def per_device(
    spectrum, core_tensor, input_factor, output_factor, first_factor, second_factor, third_factor
):
    everyone = ("mx", "my", "col")
    count = lax.axis_size("my")
    seconds = [second_factor]
    for k in range(1, 4):
        pairs = [(b, b ^ k) for b in range(count)]
        seconds.append(lax.ppermute(second_factor, "my", pairs))
    core = jnp.transpose(core_tensor, (0, 1, 3, 4, 5, 2)).reshape(2, 8, 256, 64)
    spec = spectrum.reshape(2, 2, 1024, LANES)
    chunks, halves, by_z = spectrum_chunks(spec, core, input_factor.T, first_factor, third_factor)
    chunks = core_chunks(chunks, halves, by_z, seconds)
    got = swap(chunks.reshape(128, 1, CHUNK * LANES), everyone)
    values = mode_products(got.reshape(128 * CHUNK, LANES))
    values = swap(values.reshape(128, 16, LANES), everyone)
    out = output_modes(values.reshape(2048, LANES), output_factor.T)
    return out.reshape(spectrum.shape)


def solution(mesh):
    placed = (
        P(None, "col", None, "mx", "my"),
        P(None, "col", None, ("mx", "my"), None, None),
        P(),
        P(),
        P("mx", None),
        P("my", None),
        P(),
    )
    return jax.shard_map(
        per_device,
        mesh=mesh,
        in_specs=placed,
        out_specs=P(None, "col", None, "mx", "my"),
        check_vma=False,
    )
```

```python
import jax
import jax.numpy as jnp
from jax import lax
from jax.experimental import pallas as pl
from jax.experimental.pallas import tpu as pltpu
from jax.sharding import PartitionSpec as P


LANES = 128
CHUNK = 49
WIDE = 65
VMEM_SMALL = 16 * 2**20
VMEM_LARGE = 32 * 2**20


def dot(a, b):
    return jnp.dot(a, b, preferred_element_type=jnp.float32)


def split(x):
    high = x.astype(jnp.bfloat16)
    return high, (x - high.astype(jnp.float32)).astype(jnp.bfloat16)


def split3(x):
    high = x.astype(jnp.bfloat16)
    return (high, *split(x - high.astype(jnp.float32)))


def iota(shape, dim):
    return lax.broadcasted_iota(jnp.int32, shape, dim)


def pick(rows, chosen, table):
    shape = (rows, 3 * table.shape[0])
    one = chosen(iota(shape, 0), iota(shape, 1) & (table.shape[0] - 1)).astype(jnp.bfloat16)
    return dot(one, jnp.concatenate(split3(table), axis=0))


def pick_lanes(table, lanes, chosen):
    shape = (3 * table.shape[1], lanes)
    one = chosen(iota(shape, 0) & (table.shape[1] - 1), iota(shape, 1)).astype(jnp.bfloat16)
    return dot(jnp.concatenate(split3(table), axis=1), one)


def spectrum_kernel(
    spec_ref, core_ref, in_ref, first_ref, third_ref, out_ref, half_ref, by_z_ref
):
    mine = pick_lanes(first_ref[...], 128, lambda row, col: col & 15 == row)
    mine = jnp.where(iota((8, 128), 1) >> 4 == iota((8, 128), 0), mine, 0.0)
    mine = jnp.sum(mine, axis=0, keepdims=True)
    out_ref[pl.ds(48, 128, stride=CHUNK), :] = jnp.broadcast_to(mine, (128, LANES))

    high, low = split(in_ref[...])
    rows = jnp.concatenate(
        [jnp.concatenate([high, high], axis=1), jnp.concatenate([low, low], axis=1)], axis=0
    )
    third = pick_lanes(third_ref[...], 256, lambda row, col: col & 15 == row)
    by_z_ref[...] = pick(128, lambda row, col: row & 15 == col, third)
    for b in range(2):
        for k in range(8):
            both = jnp.concatenate(
                [spec_ref[part, b, pl.ds(k, 128, stride=8), :] for part in range(2)], axis=1
            )
            out = dot(rows, jnp.concatenate(split(both), axis=0))
            out = out[:64] + out[64:]
            turned = jnp.concatenate([out[:, :LANES], out[:, LANES:]], axis=0).T
            out_ref[pl.ds(2 * k + b, 128, stride=CHUNK), :] = turned
    for pair in range(4):
        both = jnp.concatenate(
            [core_ref[part, 2 * pair + half] for half in range(2) for part in range(2)], axis=1
        )
        half_ref[pair, 0], half_ref[pair, 1] = split(both)


def spectrum_chunks(spec, core, factor, first, third):
    return pl.pallas_call(
        spectrum_kernel,
        out_shape=(
            pltpu.VMEM((128 * CHUNK, LANES), jnp.float32),
            pltpu.VMEM((4, 2, 256, 256), jnp.bfloat16),
            pltpu.VMEM((128, 256), jnp.float32),
        ),
        compiler_params=pltpu.CompilerParams(vmem_limit_bytes=VMEM_SMALL),
        name="spectrum_chunks",
    )(spec, core, factor, first, third)


def choice_kernel(out_ref):
    b = lax.axis_index("my")
    row, col = iota((512, 96), 0), iota((512, 96), 1) & 31
    out_ref[...] = (((row >> 7) ^ b) * 8 + ((row & 127) >> 4) == col).astype(jnp.bfloat16)


def choices():
    return pl.pallas_call(
        choice_kernel,
        out_shape=pltpu.VMEM((512, 96), jnp.bfloat16),
        compiler_params=pltpu.CompilerParams(vmem_limit_bytes=VMEM_SMALL),
        cost_estimate=pl.CostEstimate(flops=10**10, bytes_accessed=98304, transcendentals=0),
        name="choices",
    )()


def core_kernel(_, half_ref, by_z_ref, one_ref, s0_ref, s1_ref, s2_ref, s3_ref, out_ref):
    seconds = jnp.concatenate([ref[...] for ref in (s0_ref, s1_ref, s2_ref, s3_ref)], axis=0)
    second = pick_lanes(seconds, 256, lambda row, col: col >> 4 == row)
    by_y = dot(one_ref[...], jnp.concatenate(split3(second), axis=0))
    by_z = jnp.concatenate([by_z_ref[...]] * 4, axis=0)
    mat_high, mat_low = split(by_y * by_z)
    for pair in range(4):
        high, low = half_ref[pair, 0], half_ref[pair, 1]
        out = dot(mat_high, high) + dot(mat_high, low) + dot(mat_low, high)
        for half in range(2):
            for r in range(4):
                row = 16 + (2 * pair + half) * 4 + r
                out_ref[pl.ds(row, 128, stride=CHUNK), :] = out[
                    r * 128 : (r + 1) * 128, half * LANES : (half + 1) * LANES
                ]


def core_chunks(chunks, halves, by_z, one, seconds):
    whole = pl.BlockSpec(memory_space=pltpu.VMEM)
    return pl.pallas_call(
        core_kernel,
        in_specs=[pl.BlockSpec(memory_space=pl.ANY)] + [whole] * 7,
        out_shape=pltpu.VMEM((128 * CHUNK, LANES), jnp.float32),
        input_output_aliases={0: 0},
        compiler_params=pltpu.CompilerParams(vmem_limit_bytes=VMEM_SMALL),
        name="core_chunks",
    )(chunks, halves, by_z, one, *seconds)


def mode_kernel(got, out_ref, w_ref):
    row, col = iota((128, 128), 0), iota((128, 128), 1)
    first = jnp.concatenate([got[pl.ds(a * 32 * CHUNK + 48, 1), :] for a in range(4)] * 2, axis=0)
    first = pick(128, lambda row, col: row >> 5 == col, first)
    first = jnp.where(col >> 4 == row & 7, first, 0.0)
    first = pick_lanes(first, 128, lambda row, col: row & 15 == col & 15)
    high, low = split(jnp.where((row >> 3) & 3 == (col >> 4) & 3, first, 0.0))
    expand = jnp.concatenate([high, low], axis=1)

    for pair in range(32):
        src, two = pair // 4, pair % 4
        block = jnp.concatenate(
            [
                jnp.concatenate(
                    [
                        got[pl.ds(src * CHUNK + 16 + (2 * two + half) * 4 + r, 16, stride=8 * CHUNK), :]
                        for r in range(4)
                    ],
                    axis=0,
                )
                for half in range(2)
            ],
            axis=1,
        )
        high, low = split(block)
        out = dot(expand, jnp.concatenate([high, low, high, low], axis=0))
        for half in range(2):
            w_ref[pl.ds(src * 8 + 2 * two + half, 128, stride=WIDE), :] = out[
                :, half * LANES : (half + 1) * LANES
            ]

    left = iota((16, LANES), 1) < 64
    sign = jnp.where(left, -1.0, 1.0)

    for g in range(16):
        for k in range(8):
            x = jnp.concatenate(
                [got[pl.ds(g * 8 * CHUNK + 2 * k + b, 8, stride=CHUNK), :] for b in range(2)],
                axis=0,
            )
            swapped = pltpu.roll(x, 64, 1)
            real, imag = jnp.where(left, x, swapped), jnp.where(left, swapped, x)
            rows = jnp.concatenate([*split(real), *split(imag)], axis=0)
            w = w_ref[pl.ds((g * 8 + k) * WIDE, 64), :]
            out = dot(rows, jnp.concatenate(split(w), axis=0))
            by_real, by_imag = out[:16] + out[16:32], out[32:48] + out[48:]
            swapped = pltpu.roll(by_imag, 64, 1)
            value = by_real + sign * swapped
            for b in range(2):
                out_ref[pl.ds(g * 128 + 2 * k + b, 8, stride=16), :] = value[b * 8 : (b + 1) * 8]


def mode_products(got):
    return pl.pallas_call(
        mode_kernel,
        out_shape=jax.ShapeDtypeStruct((128 * 16, LANES), jnp.float32),
        scratch_shapes=[pltpu.VMEM((128 * WIDE, LANES), jnp.float32)],
        compiler_params=pltpu.CompilerParams(vmem_limit_bytes=VMEM_LARGE),
        name="mode_products",
    )(got)


def output_kernel(value_ref, factor_ref, out_hbm, out_ref, sems):
    high, low = split(factor_ref[...].T)
    factor = jnp.concatenate([high, high, low, low], axis=1)
    copies = [
        pltpu.make_async_copy(out_ref.at[:, b], out_hbm.at[:, b], sems.at[b]) for b in range(2)
    ]
    for b in range(2):
        for k in range(8):
            turned = value_ref[pl.ds(2 * k + b, 128, stride=16), :].T
            high, low = split(jnp.concatenate([turned[:64], turned[64:]], axis=1))
            out = dot(factor, jnp.concatenate([high, low, high, low], axis=0))
            for part in range(2):
                out_ref[part, b, pl.ds(k, 128, stride=8), :] = out[
                    :, part * LANES : (part + 1) * LANES
                ]
        copies[b].start()
    for copy in copies:
        copy.wait()


def output_modes(values, factor):
    whole = (2, 2, 1024, LANES)
    return pl.pallas_call(
        output_kernel,
        out_specs=pl.BlockSpec(memory_space=pl.ANY),
        out_shape=jax.ShapeDtypeStruct(whole, jnp.float32),
        scratch_shapes=[pltpu.VMEM(whole, jnp.float32), pltpu.SemaphoreType.DMA((2,))],
        compiler_params=pltpu.CompilerParams(vmem_limit_bytes=VMEM_SMALL),
        name="output_modes",
    )(values, factor)


def swap(chunks, axes):
    return lax.all_to_all(chunks, axes, split_axis=0, concat_axis=0, tiled=True)


def per_device(
    spectrum, core_tensor, input_factor, output_factor, first_factor, second_factor, third_factor
):
    everyone = ("mx", "my", "col")
    count = lax.axis_size("my")
    one = choices()
    seconds = [second_factor]
    for k in range(1, 4):
        pairs = [(b, b ^ k) for b in range(count)]
        seconds.append(lax.ppermute(second_factor, "my", pairs))
    core = jnp.transpose(core_tensor, (0, 1, 3, 4, 5, 2)).reshape(2, 8, 256, 64)
    spec = spectrum.reshape(2, 2, 1024, LANES)
    chunks, halves, by_z = spectrum_chunks(spec, core, input_factor.T, first_factor, third_factor)
    chunks = core_chunks(chunks, halves, by_z, one, seconds)
    got = swap(chunks.reshape(128, 1, CHUNK * LANES), everyone)
    values = mode_products(got.reshape(128 * CHUNK, LANES))
    values = swap(values.reshape(128, 16, LANES), everyone)
    out = output_modes(values.reshape(2048, LANES), output_factor.T)
    return out.reshape(spectrum.shape)


def solution(mesh):
    placed = (
        P(None, "col", None, "mx", "my"),
        P(None, "col", None, ("mx", "my"), None, None),
        P(),
        P(),
        P("mx", None),
        P("my", None),
        P(),
    )
    return jax.shard_map(
        per_device,
        mesh=mesh,
        in_specs=placed,
        out_specs=P(None, "col", None, "mx", "my"),
        check_vma=False,
    )
```
